128 devices in a mesh: gx: 8 (over z, core), gy: 4 (over x), lev: 4 (over y).
Axes of the slice: x: 4, y: 4, z: 4, core: 2. Of those that a mesh axis runs over, the one named last changes fastest.
Arguments:
- u_wind: float32 [256, 128, 512], P('lev', 'gx', 'gy'), may hold values from -6 to 6
- v_wind: float32 [256, 128, 512], P('lev', 'gx', 'gy'), may hold values from -6 to 6
- w_wind: float32 [256, 128, 512], P('lev', 'gx', 'gy'), may hold values from -4 to 4
- pressure: float32 [256, 128, 512], P('lev', 'gx', 'gy'), may hold values from -6 to 6
- buoyancy: float32 [256, 128, 512], P('lev', 'gx', 'gy'), may hold values from 0.5 to 2
- stiffness: float32 [256, 128, 512], P('lev', 'gx', 'gy'), may hold values from 0.5 to 2
Outputs:
- u_final: float32 [256, 128, 512], P('lev', 'gx', 'gy')
- v_final: float32 [256, 128, 512], P('lev', 'gx', 'gy')
- w_final: float32 [256, 128, 512], P('lev', 'gx', 'gy')
- p_final: float32 [256, 128, 512], P('lev', 'gx', 'gy')
The draws below stay inside these ranges and needn't reach their ends.
All inputs are finite; a program needn't handle non-finite values.
Results may differ from the reference program's by a relative error of at most 0.002.
Values sent between devices are 32-bit elements; how exact they have to be, the bound alone decides.
No kernel may reach another device: no remote copies, remote signals or barrier semaphores. Data moves between devices by JAX's collectives and lax.ppermute only.
A program may use at most 128 MiB of HBM per device.

```python
import math
import jax
import jax.numpy as jnp
from jax import lax

SUBSTEPS = 3
NX = 128
NY = 512
NZ = 256


def draw_w_wind(key, part):
    walk_key, rough_key = jax.random.split(jax.random.fold_in(key, 11))
    grid_shape = (NZ, NX, NY)
    increments = jax.random.normal(walk_key, grid_shape, jnp.float32)
    random_walk = jnp.cumsum(increments, axis=0) / jnp.sqrt(jnp.float32(NZ))
    rough_part = 0.3 * jax.random.normal(rough_key, grid_shape, jnp.float32)
    return jnp.clip(random_walk + rough_part, -4.0, 4.0)


def levels(own_key, extent, cuts, least, largest):
    factor_of, own = 1.0, jax.random.fold_in(own_key, 6)
    for axis_at, blocks in cuts:
        draws = jnp.exp(jax.random.uniform(jax.random.fold_in(own, axis_at), (blocks,), jnp.float32, least / len(cuts), largest / len(cuts)))
        factor_of = factor_of * jnp.repeat(draws, extent[axis_at] // blocks).reshape([-1 if axis == axis_at else 1 for axis in range(len(extent))])
    return factor_of


def scatter_about(stream_key, dims, deviation, reach, cuts=(), kind=jnp.bfloat16):
    loudness = levels(stream_key, dims, cuts, -0.22, 0.18) if cuts else 1.0
    drawn = jax.random.normal(stream_key, dims, jnp.float32) * deviation * loudness
    return jnp.minimum(jnp.maximum(drawn, -reach), reach).astype(kind)


def setup_inputs(seed: int = 0) -> dict:
    streams_of = jax.random.split(jax.random.key(seed), 7)
    u_wind = scatter_about(streams_of[0], (NZ, NX, NY), 1.0, 6.0, ((0, 4), (1, 8), (2, 4)), jnp.float32)
    v_wind = scatter_about(streams_of[1], (NZ, NX, NY), 1.0, 6.0, ((0, 4), (1, 8), (2, 4)), jnp.float32)
    w_wind = draw_w_wind(jax.random.fold_in(streams_of[6], 71), 0)
    pressure = scatter_about(streams_of[3], (NZ, NX, NY), 1.0, 6.0, ((0, 4), (1, 8), (2, 4)), jnp.float32)
    buoyancy = jnp.clip(jnp.exp(math.log(2.0) - 1.3862944 * jax.random.uniform(streams_of[4], (NZ, NX, NY), jnp.float32) ** levels(streams_of[4], (NZ, NX, NY), ((0, 4), (1, 8), (2, 4)), -0.2, 0.2)), 0.5, 2.0)
    stiffness = jnp.clip(jnp.exp(math.log(2.0) - 1.3862944 * jax.random.uniform(streams_of[5], (NZ, NX, NY), jnp.float32) ** levels(streams_of[5], (NZ, NX, NY), ((0, 4), (1, 8), (2, 4)), -0.2, 0.2)), 0.5, 2.0)
    return dict(u_wind=u_wind, v_wind=v_wind, w_wind=w_wind, pressure=pressure, buoyancy=buoyancy, stiffness=stiffness)


courant_h = 0.3
vertical_gain = 4096.0

def neighbour(grid_field, offset, axis_number):
    return jnp.roll(grid_field, -offset, axis=axis_number)

def reference(u_wind, v_wind, w_wind, pressure, buoyancy, stiffness):
    zero_row = jnp.zeros((1,) + pressure.shape[1:], jnp.float32)
    stiff_up = jnp.concatenate([stiffness[1:], zero_row], 0)
    lower_band = -vertical_gain * buoyancy * stiffness
    lower_band = jnp.concatenate([zero_row, lower_band[1:]], 0)
    upper_band = -vertical_gain * buoyancy * stiff_up
    main_band = 1.0 + vertical_gain * buoyancy * (stiffness + stiff_up)
    lower_cols = jnp.moveaxis(lower_band, 0, -1)
    main_cols = jnp.moveaxis(main_band, 0, -1)
    upper_cols = jnp.moveaxis(upper_band, 0, -1)
    for substep in range(SUBSTEPS):
        u_new = u_wind - courant_h * buoyancy * (neighbour(pressure, 1, 1) - neighbour(pressure, -1, 1))
        v_new = v_wind - courant_h * buoyancy * (neighbour(pressure, 1, 2) - neighbour(pressure, -1, 2))
        divergence = neighbour(u_new, 1, 1) - neighbour(u_new, -1, 1) + (neighbour(v_new, 1, 2) - neighbour(v_new, -1, 2))
        p_star = pressure - courant_h * stiffness * divergence
        p_above = jnp.concatenate([p_star[1:], zero_row], 0)
        right_side = w_wind - vertical_gain * buoyancy * (p_above - p_star)
        solved = lax.linalg.tridiagonal_solve(lower_cols, main_cols, upper_cols, jnp.moveaxis(right_side, 0, -1)[..., None])
        w_new = jnp.moveaxis(solved[..., 0], -1, 0)
        w_below = jnp.concatenate([zero_row, w_new[:-1]], 0)
        pressure = p_star - stiffness * (w_new - w_below)
        u_wind, v_wind, w_wind = (u_new, v_new, w_new)
    return (u_wind, v_wind, w_wind, pressure)
```

```python
import functools

import jax
import jax.numpy as jnp
from jax import lax
from jax.experimental import pallas as pl
from jax.experimental.pallas import tpu as pltpu
from jax.sharding import PartitionSpec as P

SUBSTEPS = 3

courant_h = 0.3
vertical_gain = 4096.0

F32 = jnp.float32
NI, NK, NL = 16, 64, 128
TK = NK // 8


def level(k):
    return pl.ds(NI * k, NI)


def level_ik(k):
    return pl.ds(k, NI, stride=NK)


def row(i):
    return pl.ds(NK * i, NK)


def row_ki(i):
    return pl.ds(i, NK, stride=NI)


def vmem(*shape):
    return pltpu.VMEM(shape, F32)


BLOCK = (NI * NK, NL)
PACK = (4 * 8, NL)


def call(body, outs, args, name):
    whole = pl.BlockSpec(memory_space=pltpu.VMEM)
    args = [pltpu.with_memory_space_constraint(x, pltpu.VMEM) for x in args]
    return pl.pallas_call(
        body,
        out_shape=tuple(vmem(*shape) for shape in outs),
        in_specs=[whole] * len(args),
        out_specs=(whole,) * len(outs),
        name=name,
        compiler_params=pltpu.CompilerParams(vmem_limit_bytes=2 << 20),
    )(*args)


def pack_edges(field, pack, at):
    lane = lax.broadcasted_iota(jnp.int32, (8, NL), 1) // 4
    for group in range(4):
        packed = jnp.zeros((8, NL), F32)
        for tile in range(32):
            i, kt = group * 4 + tile // 8, tile % 8
            rolled = pltpu.roll(field[pl.ds(NK * i + 8 * kt, 8), :], 4 * tile + 2, 1)
            packed = jnp.where(lane == tile, rolled, packed)
        pack[pl.ds(at + 8 * group, 8), :] = packed


def unpacked(packs, i):
    source = packs[8 * (i // 4) : 8 * (i // 4) + 8]
    parts = []
    for kt in range(TK):
        base = 4 * ((i % 4) * 8 + kt) + 2
        parts.append(pltpu.roll(source, (NL - base) % NL, 1))
    return jnp.concatenate(parts, 0)


def prologue(p_in, u_in, v_in, b_in, p, u, v, b, to_up, to_down, edges):
    for source, target in ((p_in, p), (u_in, u), (v_in, v), (b_in, b)):
        for i in range(NI):
            target[row(i), :] = source[row_ki(i), :]
    for at, (field, i) in enumerate(((p, 14), (p, 15), (u, 15), (b, 15))):
        to_up[row(at), :] = field[row(i), :]
    for at, (field, i) in enumerate(((p, 0), (p, 1), (u, 0), (b, 0))):
        to_down[row(at), :] = field[row(i), :]
    for at, field in enumerate((p, v, b)):
        pack_edges(field, edges, 32 * at)


def factor(b_in, s_in, w_in, s, theta, rest, g_out, eta, inv, t1, y1, a_p, top_p, a_w, top_w, statics, sums):
    for i in range(NI):
        s[row(i), :] = s_in[row_ki(i), :]
    first = s_in[level(0), :]
    passed = first
    held = None
    for k in range(NK):
        g = 1.0 / (vertical_gain * b_in[level(k), :])
        g_out[level(k), :] = g
        if k == 0:
            c = first
        else:
            stiff = s_in[level(k), :]
            ratio = 1.0 / (held + stiff)
            th = held * ratio
            rs = stiff * ratio
            theta[level(k), :] = th
            rest[level(k), :] = rs
            c = stiff * th
            passed = passed * rs
        held = g + c
        ic = 1.0 / held
        inv[level(k), :] = ic
        eta[level(k), :] = c * ic
        t1[level(k), :] = (g * ic) * passed
        y1[level(k), :] = passed * ic
    theta[level(0), :] = jnp.ones((NI, NL), F32)
    rest[level(0), :] = jnp.zeros((NI, NL), F32)
    statics[level(1), :] = passed
    statics[level(2), :] = held
    weight = jnp.ones((NI, NL), F32)
    above = jnp.zeros((NI, NL), F32)
    reply_above = None
    sum_a = jnp.zeros((NI, NL), F32)
    sum_t = jnp.zeros((NI, NL), F32)
    for k in range(NK - 1, -1, -1):
        g = g_out[level(k), :]
        w = w_in[level(k), :]
        top_p[level_ik(k), :] = theta[level(k), :] * weight
        gw = g * weight
        top_w[level(k), :] = gw
        sum_t = sum_t + gw * w
        weight = weight * rest[level(k), :]
        reply = y1[level(k), :] - inv[level(k), :] * above
        above = t1[level(k), :] + eta[level(k), :] * above
        gr = g * reply
        a_w[level(k), :] = gr
        sum_a = sum_a - gr * w
        if reply_above is not None:
            a_p[level_ik(k + 1), :] = reply - reply_above
        reply_above = reply
    a_p[level_ik(0), :] = 1.0 - reply_above
    statics[level(0), :] = above
    sums[level(0), :] = sum_a
    sums[level(1), :] = sum_t


def explicit(first, last, *refs):
    (p, u, v, b, s, a_p, top_p, sums, own, low, high, left, right, low0, high0, left0, right0), refs = refs[:17], refs[17:]
    if first:
        statics, refs = refs[0], refs[1:]
        u_low, u_high = low0[row(2), :], high0[row(2), :]
    else:
        (u_halo, v_halo), refs = refs[:2], refs[2:]
        u_low, u_high = u_halo[row(0), :], u_halo[row(1), :]
    u_new, v_new, p_star, message = refs[:4]
    u_next = list(refs[4:])
    lane = lax.broadcasted_iota(jnp.int32, PACK, 1) % 4
    low_slot = lane == 2
    joined = lambda from_left, from_right, by: jnp.where(
        low_slot, pltpu.roll(from_left, by, 1), pltpu.roll(from_right, NL - by, 1)
    )
    near = joined(left[0:32, :], right[0:32, :], 1)
    far = joined(left[0:32, :], right[0:32, :], 2)
    b_side = joined(left0[64:96, :], right0[64:96, :], 1)
    v_side = joined(left0[32:64, :], right0[32:64, :], 1) if first else v_halo[...]
    gap = own[0:32, :] - far
    v_side = v_side - courant_h * b_side * jnp.where(low_slot, gap, -gap)
    p_low2, p_low1 = low[row(0), :], low[row(1), :]
    p_high1, p_high2 = high[row(0), :], high[row(1), :]
    u_low = u_low - courant_h * low0[row(3), :] * (p[row(0), :] - p_low2)
    u_high = u_high - courant_h * high0[row(3), :] * (p_high2 - p[row(NI - 1), :])
    if not last:
        u_next[0][row(0), :] = u_low
        u_next[0][row(1), :] = u_high
        u_next[1][...] = v_side
    lane = lax.broadcasted_iota(jnp.int32, (NK, NL), 1)
    ends = (lane == 0, lane == NL - 1)

    def difference(x, halo):
        up = jnp.where(ends[1], halo, pltpu.roll(x, NL - 1, 1))
        down = jnp.where(ends[0], halo, pltpu.roll(x, 1, 1))
        return up - down

    def u_row(i):
        above = p_high1 if i == NI - 1 else p[row(i + 1), :]
        below = p_low1 if i == 0 else p[row(i - 1), :]
        return u[row(i), :] - courant_h * b[row(i), :] * (above - below)

    before, here = u_low, u_row(0)
    for i in range(NI):
        after = u_high if i == NI - 1 else u_row(i + 1)
        pressure = p[row(i), :]
        vn = v[row(i), :] - courant_h * b[row(i), :] * difference(pressure, unpacked(near, i))
        divergence = (after - before) + difference(vn, unpacked(v_side, i))
        star = pressure - courant_h * s[row(i), :] * divergence
        if last:
            u_new[row_ki(i), :] = here
            v_new[row_ki(i), :] = vn
        else:
            u_new[row(i), :] = here
            v_new[row(i), :] = vn
        p_star[row_ki(i), :] = star
        message[pl.ds(i, 1), :] = sums[pl.ds(i, 1), :] + jnp.sum(a_p[row(i), :] * star, 0, keepdims=True)
        message[pl.ds(NI + i, 1), :] = sums[pl.ds(NI + i, 1), :] + jnp.sum(top_p[row(i), :] * star, 0, keepdims=True)
        before, here = here, after
    if first:
        message[pl.ds(2 * NI, 3 * NI), :] = statics[...]


def upward(p_star, w, theta, rest, g_in, eta, inv, t0, y0):
    carried = None
    for k in range(NK):
        star = p_star[level(k), :]
        gw = g_in[level(k), :] * w[level(k), :]
        if k == 0:
            carried = star
        else:
            carried = theta[level(k), :] * star + rest[level(k), :] * (carried + held_gw)
        held_gw = gw
        e = eta[level(k), :]
        t0[level(k), :] = carried - e * (carried + gw)
        y0[level(k), :] = (carried + gw) * inv[level(k), :]


def interface(position, by_group, statics):
    a = [x[0:NI] for x in by_group]
    top = [x[NI : 2 * NI] for x in by_group]
    kappa, scale, shifted, reach, conduct = statics
    tops = [top[0]]
    for m in range(2):
        tops.append(scale[m] * top[m + 1] + shifted[m] * (tops[m] - a[m + 1]))
    y_above = jnp.zeros((NI, NL), F32)
    xs, ys = [None] * 3, [None] * 3
    for m in (2, 1, 0):
        xs[m] = kappa[m] * (tops[m] - a[m + 1] - (reach[m] * y_above if m < 2 else 0.0))
        ys[m] = tops[m] - conduct[m] * xs[m]
        y_above = ys[m]
    zero = jnp.zeros((NI, NL), F32)
    w_low = jnp.where(position == 0, zero, jnp.where(position == 1, xs[0], jnp.where(position == 2, xs[1], xs[2])))
    p_high = jnp.where(position == 3, zero, jnp.where(position == 2, ys[2], jnp.where(position == 1, ys[1], ys[0])))
    return w_low, p_high


def reduced_statics(by_group):
    beta = [x[2 * NI : 3 * NI] for x in by_group]
    phi = [x[3 * NI : 4 * NI] for x in by_group]
    grounded = [x[4 * NI : 5 * NI] for x in by_group]
    conduct = [grounded[0]]
    kappa, scale, shifted, reach = [], [], [], []
    for m in range(3):
        kappa.append(1.0 / (conduct[m] + beta[m + 1]))
        reach.append(phi[m + 1] / grounded[m + 1])
        if m < 2:
            coupled = phi[m + 1] * kappa[m]
            scale.append(1.0 / (1.0 + coupled * reach[m]))
            shifted.append(coupled * scale[m])
            conduct.append(grounded[m + 1] * scale[m])
    return kappa, scale, shifted, reach, conduct


COUNTS = (3, 2, 2, 3, 3)


def implicit(first, last, *refs):
    (t0, y0, t1, y1, eta, inv, own, by1, by2, by3), refs = refs[:10], refs[10:]
    if not first:
        kept, refs = refs[0], refs[1:]
    if not last:
        (a_w, top_w), refs = refs[:2], refs[2:]
    w, p = refs[:2]
    if not last:
        sums, to_up, to_down, edges = refs[2:6]
    position = lax.axis_index("lev")
    others = [ref[...] for ref in (own, by1, by2, by3)]
    by_group = []
    for group in range(4):
        mask = position ^ group
        by_group.append(
            jnp.where(mask == 0, others[0], jnp.where(mask == 1, others[1], jnp.where(mask == 2, others[2], others[3])))
        )
    if first:
        statics = reduced_statics(by_group)
        keep, at = refs[6], 0
        for family in statics:
            for member in family:
                keep[level(at), :] = member
                at += 1
    else:
        statics, at = [], 0
        for count in COUNTS:
            statics.append([kept[level(at + m), :] for m in range(count)])
            at += count
    w_low, p_high = interface(position, by_group, statics)
    above = p_high
    sum_a = jnp.zeros((NI, NL), F32)
    sum_t = jnp.zeros((NI, NL), F32)
    for k in range(NK - 1, -1, -1):
        wn = y0[level(k), :] + y1[level(k), :] * w_low - inv[level(k), :] * above
        above = t0[level(k), :] + t1[level(k), :] * w_low + eta[level(k), :] * above
        w[level(k), :] = wn
        if last:
            p[level(k), :] = above
        else:
            p[level_ik(k), :] = above
            sum_a = sum_a - a_w[level(k), :] * wn
            sum_t = sum_t + top_w[level(k), :] * wn
    if not last:
        sums[level(0), :] = sum_a
        sums[level(1), :] = sum_t
        to_up[...] = p[pl.ds(14 * NK, 2 * NK), :]
        to_down[...] = p[pl.ds(0, 2 * NK), :]
        pack_edges(p, edges, 0)


def ring(block, axis, distance):
    size = lax.axis_size(axis)
    return lax.ppermute(block, axis, [(i, (i + distance) % size) for i in range(size)])


def partner(block, mask):
    return lax.ppermute(block, "lev", [(i, i ^ mask) for i in range(4)])


def shards(u_wind, v_wind, w_wind, pressure, buoyancy, stiffness):
    u_in, v_in, w, p_in, b_in, s_in = (
        x.reshape(BLOCK) for x in (u_wind, v_wind, w_wind, pressure, buoyancy, stiffness)
    )
    p, u, v, b, to_up, to_down, edges = call(
        prologue,
        [BLOCK] * 4 + [(4 * NK, NL), (4 * NK, NL), (96, NL)],
        [p_in, u_in, v_in, b_in],
        "prologue",
    )
    (s, theta, rest, g, eta, inv, t1, y1, a_p, top_p, a_w, top_w, statics, sums) = call(
        factor, [BLOCK] * 12 + [(3 * NI, NL), (2 * NI, NL)], [b_in, s_in, w], "factor"
    )
    halos0 = kept = u_halo = v_halo = None
    for step in range(SUBSTEPS):
        first, last = step == 0, step == SUBSTEPS - 1
        low, high = ring(to_up, "gx", 1), ring(to_down, "gx", -1)
        left, right = ring(edges, "gy", 1), ring(edges, "gy", -1)
        if first:
            halos0 = [low, high, left, right]
        args = [p, u, v, b, s, a_p, top_p, sums, edges, low, high, left, right] + halos0
        args += [statics] if first else [u_halo, v_halo]
        outs = [BLOCK] * 3 + [((5 if first else 2) * NI, NL)]
        outs += [] if last else [(2 * NK, NL), PACK]
        u, v, p_star, message, *halos = call(
            functools.partial(explicit, first, last), outs, args, f"explicit{step}"
        )
        if not last:
            u_halo, v_halo = halos
        others = [partner(message, mask) for mask in (1, 2, 3)]
        t0, y0 = call(upward, [BLOCK] * 2, [p_star, w, theta, rest, g, eta, inv], f"upward{step}")
        args = [t0, y0, t1, y1, eta, inv, message] + others
        args += [] if first else [kept]
        args += [] if last else [a_w, top_w]
        outs = [BLOCK] * 2
        if not last:
            outs += [(2 * NI, NL), (2 * NK, NL), (2 * NK, NL), PACK]
        if first:
            outs += [(sum(COUNTS) * NI, NL)]
        w, p, *more = call(functools.partial(implicit, first, last), outs, args, f"implicit{step}")
        if not last:
            sums, to_up, to_down, edges, *more = more
        if first:
            kept = more[0]
    return tuple(x.reshape(NK, NI, NL) for x in (u, v, w, p))


def solution(mesh):
    return jax.shard_map(
        shards,
        mesh=mesh,
        in_specs=(P("lev", "gx", "gy"),) * 6,
        out_specs=(P("lev", "gx", "gy"),) * 4,
        check_vma=False,
    )
```

```python
import functools

import jax
import jax.numpy as jnp
from jax import lax
from jax.experimental import pallas as pl
from jax.experimental.pallas import tpu as pltpu
from jax.sharding import PartitionSpec as P

SUBSTEPS = 3

courant_h = 0.3
vertical_gain = 4096.0

F32 = jnp.float32
NI, NK, NL = 16, 64, 128

STEP = 24
PADDED = ((NK + 1) * STEP, NL)
BLOCK = (NI * NK, NL)
PACK = (4 * 8, NL)


def level(k):
    return pl.ds(NI * k, NI)


def row(i):
    return pl.ds(NK * i, NK)


def padded_row(i):
    return pl.ds(8 + i, NK, stride=STEP)


def vmem(*shape):
    return pltpu.VMEM(shape, F32)


def hbm(*shape):
    return pltpu.HBM(shape, F32)


def call(body, outs, args, name, scratch=(), aliases=None, far_in=0, far_out=0, limit=2):
    near, far = pl.BlockSpec(memory_space=pltpu.VMEM), pl.BlockSpec(memory_space=pltpu.HBM)
    args = [
        pltpu.with_memory_space_constraint(x, pltpu.HBM if at < far_in else pltpu.VMEM) for at, x in enumerate(args)
    ]
    return pl.pallas_call(
        body,
        out_shape=tuple((hbm if at < far_out else vmem)(*shape) for at, shape in enumerate(outs)),
        in_specs=[far] * far_in + [near] * (len(args) - far_in),
        out_specs=(far,) * far_out + (near,) * (len(outs) - far_out),
        scratch_shapes=list(scratch),
        input_output_aliases=aliases or {},
        name=name,
        compiler_params=pltpu.CompilerParams(vmem_limit_bytes=limit << 20),
    )(*args)


def tiles():
    for group in range(4):
        for tile in range(32):
            yield group, tile, group * 16 + tile // 2, 8 * (tile % 2)


def pack_edges(load):
    lane = lax.broadcasted_iota(jnp.int32, (8, NL), 1) // 4
    packs = [jnp.zeros((8, NL), F32)] * 4
    for group, tile, k, i in tiles():
        rolled = pltpu.roll(load(k, i), 4 * tile + 2, 1)
        packs[group] = jnp.where(lane == tile, rolled, packs[group])
    return jnp.concatenate(packs, 0)


def slots(shape=PACK):
    return lax.broadcasted_iota(jnp.int32, shape, 1) % 4


def turn(x, by):
    return pltpu.roll(x, by % NL, 1)


def block_row(i):
    return pl.ds(i, NK, stride=NI)


def prologue(p_in, v_in, b_in, u_in, p, v, b, u, to_up, to_down, to_right, to_left, sems):
    copies = []
    for at, (source, target) in enumerate(((p_in, p), (v_in, v), (b_in, b), (u_in, u))):
        copies.append(pltpu.make_async_copy(source, target, sems.at[at]))
    for copy in copies:
        copy.start()
    packs = []
    for copy, field in zip(copies, (p, v, b)):
        copy.wait()
        packs.append(pack_edges(lambda k, i: field[pl.ds(NI * k + i, 8), :]))
    edge_p, edge_v, edge_b = packs
    slot = slots()
    to_right[...] = jnp.where(slot < 2, edge_p, jnp.where(slot == 2, turn(edge_v, 1), turn(edge_b, 2)))
    to_left[...] = jnp.where(slot < 2, turn(edge_p, -2), jnp.where(slot == 2, edge_v, turn(edge_b, 1)))
    copies[3].wait()
    for at, (field, i) in enumerate(((p, 14), (p, 15), (u, 15), (b, 15))):
        to_up[row(at), :] = field[block_row(i), :]
    for at, (field, i) in enumerate(((p, 0), (p, 1), (u, 0), (b, 0))):
        to_down[row(at), :] = field[block_row(i), :]


def factor(
    s_in, w_in, b_in, v_in,
    theta, rest, g_out, eta, inv, t1, y1, a_p, top_p, a_w, top_w, v, b_v, statics, sums,
):
    first = s_in[level(0), :]
    passed = first
    held = None
    for k in range(NK):
        v[level(k), :] = turn(v_in[level(k), :], -1)
        b_v[level(k), :] = turn(b_in[level(k), :], -1)
        g = 1.0 / (vertical_gain * b_in[level(k), :])
        g_out[level(k), :] = g
        stiff = s_in[level(k), :]
        if k == 0:
            c = first
        else:
            ratio = 1.0 / (held + stiff)
            th = held * ratio
            rs = stiff * ratio
            theta[level(k), :] = th
            rest[level(k), :] = rs
            c = stiff * th
            passed = passed * rs
        held = g + c
        ic = 1.0 / held
        inv[level(k), :] = ic
        eta[level(k), :] = c * ic
        t1[level(k), :] = (g * ic) * passed
        y1[level(k), :] = passed * ic
    theta[level(0), :] = jnp.ones((NI, NL), F32)
    rest[level(0), :] = jnp.zeros((NI, NL), F32)
    statics[level(1), :] = passed
    statics[level(2), :] = held
    weight = jnp.ones((NI, NL), F32)
    above = jnp.zeros((NI, NL), F32)
    reply_above = None
    sum_a = jnp.zeros((NI, NL), F32)
    sum_t = jnp.zeros((NI, NL), F32)
    for k in range(NK - 1, -1, -1):
        g = g_out[level(k), :]
        w = w_in[level(k), :]
        top_p[level(k), :] = theta[level(k), :] * weight
        gw = g * weight
        top_w[level(k), :] = gw
        sum_t = sum_t + gw * w
        weight = weight * rest[level(k), :]
        reply = y1[level(k), :] - inv[level(k), :] * above
        above = t1[level(k), :] + eta[level(k), :] * above
        gr = g * reply
        a_w[level(k), :] = gr
        sum_a = sum_a - gr * w
        if reply_above is not None:
            a_p[level(k + 1), :] = reply - reply_above
        reply_above = reply
    a_p[level(0), :] = 1.0 - reply_above
    statics[level(0), :] = above
    sums[level(0), :] = sum_a
    sums[level(1), :] = sum_t


BATCH = 8


def explicit(first, last, *refs):
    (p, u, v, b_u, b_v, s, a_p, top_p, sums, own, low, high, left, right, low0, high0, extra), refs = refs[:17], refs[17:]
    if not first:
        u_sides, refs = refs[0], refs[1:]
    (u_out, v_out, p_star, message), refs = refs[:4], refs[4:]
    if first:
        b_patched, refs = refs[0], refs[1:]
    if not last:
        (side, u_side), refs = refs[:2], refs[2:]
    p_pad, u_pad = refs
    for k in range(NK):
        p_pad[pl.ds(STEP * k + 8, NI), :] = p[level(k), :]
    for i, (source, at) in ((-2, (low, 0)), (-1, (low, 1)), (NI, (high, 0)), (NI + 1, (high, 1))):
        p_pad[padded_row(i), :] = source[row(at), :]
    for n, (i, source, old) in enumerate(((-1, low, low0), (NI, high, high0))):
        held = old[row(2), :] if first else u_sides[row(n), :]
        away = 1 if n == 0 else -1
        gap = away * (p[block_row(0 if n == 0 else NI - 1), :] - source[row(0 if n == 0 else 1), :])
        held = held - courant_h * old[row(3), :] * gap
        u_pad[padded_row(i), :] = held
        if not last:
            u_side[row(n), :] = held
    slot = slots()
    from_left = turn(left[...], 2)
    if first:
        mine = own[...]
        edge = turn(mine, 2)
        v_side = jnp.where(slot == 2, left[...], turn(mine, 1))
        b_side = jnp.where(slot == 2, turn(left[...], -1), mine)
        from_right = right[...]
    else:
        edge = own[...]
        v_side, b_side = extra[pl.ds(0, 32), :], extra[pl.ds(32, 32), :]
        from_right = turn(right[...], -2)
    v_side = v_side - courant_h * b_side * (edge - from_left)
    packed = jnp.where(slot < 2, from_right, v_side)
    if not last:
        side[pl.ds(0, 32), :] = v_side
        side[pl.ds(32, 32), :] = b_side
    for k in range(NK):
        at = STEP * k + 8
        fresh = u[level(k), :] - courant_h * b_u[level(k), :] * (p_pad[pl.ds(at + 1, NI), :] - p_pad[pl.ds(at - 1, NI), :])
        u_pad[pl.ds(at, NI), :] = fresh
        u_out[level(k), :] = fresh
    size = NI * BATCH
    lane = lax.broadcasted_iota(jnp.int32, (size, NL), 1)

    def spread(source, by):
        return jnp.concatenate([turn(source, by - 4 * tile) for tile in spots], 0)

    total_a, total_t = sums[level(0), :], sums[level(1), :]
    for start in range(0, NK, BATCH):
        rows = pl.ds(NI * start, size)
        spots = range(2 * (start % 16), 2 * (start % 16) + 2 * BATCH)
        group = slice(8 * (start // 16), 8 * (start // 16) + 8)
        halo = spread(packed[group], -2)
        pressure, vs, bs = p[rows, :], v[rows, :], b_v[rows, :]
        if first:
            theirs = right[group, :]
            vs = jnp.where(lane == NL - 1, spread(theirs, NL - 3), vs)
            bs = jnp.where(lane == NL - 1, spread(theirs, NL - 4), bs)
            b_patched[rows, :] = bs
        p_next = jnp.where(lane >= NL - 2, halo, turn(pressure, -2))
        vn = vs - courant_h * bs * (p_next - pressure)
        dv = vn - jnp.where(lane < 2, halo, turn(vn, 2))
        if last:
            ahead = spread(packed[group], -4)
            v_out[rows, :] = turn(jnp.where(lane == NL - 1, ahead, vn), 1)
        else:
            v_out[rows, :] = vn
        du = jnp.concatenate(
            [
                u_pad[pl.ds(STEP * k + 9, NI), :] - u_pad[pl.ds(STEP * k + 7, NI), :]
                for k in range(start, start + BATCH)
            ],
            0,
        )
        star = pressure - courant_h * s[rows, :] * (du + dv)
        p_star[rows, :] = star
        part_a, part_t = a_p[rows, :] * star, top_p[rows, :] * star
        for k in range(BATCH):
            total_a = total_a + part_a[NI * k : NI * k + NI]
            total_t = total_t + part_t[NI * k : NI * k + NI]
    message[level(0), :] = total_a
    message[level(1), :] = total_t
    if first:
        message[pl.ds(2 * NI, 3 * NI), :] = extra[...]


def upward(last, *refs):
    if last:
        (p_star, w, theta, rest, g_in, eta, inv, u_in, v_in), (u_far, v_far, t0, y0, sems) = refs[:9], refs[9:]
        copies = [pltpu.make_async_copy(*pair, sems.at[at]) for at, pair in enumerate(((u_in, u_far), (v_in, v_far)))]
        for copy in copies:
            copy.start()
    else:
        p_star, w, theta, rest, g_in, eta, inv, t0, y0 = refs
    carried = held_gw = None
    for k in range(NK):
        star = p_star[level(k), :]
        gw = g_in[level(k), :] * w[level(k), :]
        if k == 0:
            carried = star
        else:
            carried = theta[level(k), :] * star + rest[level(k), :] * (carried + held_gw)
        held_gw = gw
        e = eta[level(k), :]
        t0[level(k), :] = carried - e * (carried + gw)
        y0[level(k), :] = (carried + gw) * inv[level(k), :]
    if last:
        for copy in copies:
            copy.wait()


def interface(position, by_group, statics):
    a = [x[0:NI] for x in by_group]
    top = [x[NI : 2 * NI] for x in by_group]
    kappa, scale, shifted, reach, conduct = statics
    tops = [top[0]]
    for m in range(2):
        tops.append(scale[m] * top[m + 1] + shifted[m] * (tops[m] - a[m + 1]))
    y_above = jnp.zeros((NI, NL), F32)
    xs, ys = [None] * 3, [None] * 3
    for m in (2, 1, 0):
        xs[m] = kappa[m] * (tops[m] - a[m + 1] - (reach[m] * y_above if m < 2 else 0.0))
        ys[m] = tops[m] - conduct[m] * xs[m]
        y_above = ys[m]
    zero = jnp.zeros((NI, NL), F32)
    w_low = jnp.where(position == 0, zero, jnp.where(position == 1, xs[0], jnp.where(position == 2, xs[1], xs[2])))
    p_high = jnp.where(position == 3, zero, jnp.where(position == 2, ys[2], jnp.where(position == 1, ys[1], ys[0])))
    return w_low, p_high


def reduced_statics(by_group):
    beta = [x[2 * NI : 3 * NI] for x in by_group]
    phi = [x[3 * NI : 4 * NI] for x in by_group]
    grounded = [x[4 * NI : 5 * NI] for x in by_group]
    conduct = [grounded[0]]
    kappa, scale, shifted, reach = [], [], [], []
    for m in range(3):
        kappa.append(1.0 / (conduct[m] + beta[m + 1]))
        reach.append(phi[m + 1] / grounded[m + 1])
        if m < 2:
            coupled = phi[m + 1] * kappa[m]
            scale.append(1.0 / (1.0 + coupled * reach[m]))
            shifted.append(coupled * scale[m])
            conduct.append(grounded[m + 1] * scale[m])
    return kappa, scale, shifted, reach, conduct


COUNTS = (3, 2, 2, 3, 3)


def implicit(first, last, *refs):
    (t0, y0, t1, y1, eta, inv, own, by1, by2, by3), refs = refs[:10], refs[10:]
    if not first:
        kept, refs = refs[0], refs[1:]
    if last:
        w_far, p_far, w, p, sems = refs
    else:
        (a_w, top_w), (w, p, sums, to_up, to_down, edges), refs = refs[:2], refs[2:8], refs[8:]
    position = lax.axis_index("lev")
    others = [ref[...] for ref in (own, by1, by2, by3)]
    by_group = []
    for group in range(4):
        mask = position ^ group
        by_group.append(
            jnp.where(mask == 0, others[0], jnp.where(mask == 1, others[1], jnp.where(mask == 2, others[2], others[3])))
        )
    if first:
        statics = reduced_statics(by_group)
        keep, at = refs[0], 0
        for family in statics:
            for member in family:
                keep[level(at), :] = member
                at += 1
    else:
        statics, at = [], 0
        for count in COUNTS:
            statics.append([kept[level(at + m), :] for m in range(count)])
            at += count
    w_low, p_high = interface(position, by_group, statics)
    above = p_high
    sum_a = jnp.zeros((NI, NL), F32)
    sum_t = jnp.zeros((NI, NL), F32)
    copies = []
    for k in range(NK - 1, -1, -1):
        wn = y0[level(k), :] + y1[level(k), :] * w_low - inv[level(k), :] * above
        above = t0[level(k), :] + t1[level(k), :] * w_low + eta[level(k), :] * above
        w[level(k), :] = wn
        p[level(k), :] = above
        if last:
            if k % 16 == 0:
                part = pl.ds(NI * k, NI * 16)
                for source, target in ((w, w_far), (p, p_far)):
                    copy = pltpu.make_async_copy(source.at[part, :], target.at[part, :], sems.at[len(copies)])
                    copy.start()
                    copies.append(copy)
        else:
            sum_a = sum_a - a_w[level(k), :] * wn
            sum_t = sum_t + top_w[level(k), :] * wn
    for copy in copies:
        copy.wait()
    if not last:
        sums[level(0), :] = sum_a
        sums[level(1), :] = sum_t
        for at, i in enumerate((14, 15)):
            to_up[row(at), :] = p[block_row(i), :]
        for at, i in enumerate((0, 1)):
            to_down[row(at), :] = p[block_row(i), :]
        edges[...] = pack_edges(lambda k, i: p[pl.ds(NI * k + i, 8), :])


def ring(block, axis, distance):
    size = lax.axis_size(axis)
    return lax.ppermute(block, axis, [(i, (i + distance) % size) for i in range(size)])


def partner(block, mask):
    return lax.ppermute(block, "lev", [(i, i ^ mask) for i in range(4)])


def shards(u_wind, v_wind, w_wind, pressure, buoyancy, stiffness):
    w, s = w_wind.reshape(BLOCK), stiffness.reshape(BLOCK)
    p, v, b, u, to_up, to_down, to_right, own = call(
        prologue,
        [BLOCK] * 4 + [(4 * NK, NL), (4 * NK, NL), PACK, PACK],
        [x.reshape(BLOCK) for x in (pressure, v_wind, buoyancy, u_wind)],
        "prologue",
        scratch=[pltpu.SemaphoreType.DMA((4,))],
        far_in=4,
    )
    to_left = own
    (theta, rest, g, eta, inv, t1, y1, a_p, top_p, a_w, top_w, v, b_v, statics, sums) = call(
        factor, [BLOCK] * 13 + [(3 * NI, NL), (2 * NI, NL)], [s, w, b, v], "factor"
    )
    extra, u_side = [statics], []
    for step in range(SUBSTEPS):
        first, last = step == 0, step == SUBSTEPS - 1
        low, high = ring(to_up, "gx", 1), ring(to_down, "gx", -1)
        left, right = ring(to_right, "gy", 1), ring(to_left, "gy", -1)
        if first:
            gx_first = [low, high]
        outs = [BLOCK] * 3 + [((5 if first else 2) * NI, NL)]
        outs += [BLOCK] if first else []
        outs += [] if last else [(2 * PACK[0], NL), (2 * NK, NL)]
        u, v, p_star, message, *more = call(
            functools.partial(explicit, first, last),
            outs,
            [p, u, v, b, b_v, s, a_p, top_p, sums, own, low, high, left, right] + gx_first + extra + u_side,
            f"explicit{step}",
            scratch=[vmem(*PADDED), vmem(*PADDED)],
            limit=3,
        )
        if first:
            b_v, *more = more
        if not last:
            extra, u_side = more[:1], more[1:]
        others = [partner(message, mask) for mask in (1, 2, 3)]
        args = [p_star, w, theta, rest, g, eta, inv]
        if last:
            u_far, v_far, t0, y0 = call(
                functools.partial(upward, True),
                [BLOCK] * 4,
                args + [u, v],
                f"upward{step}",
                scratch=[pltpu.SemaphoreType.DMA((2,))],
                far_out=2,
            )
        else:
            t0, y0 = call(functools.partial(upward, False), [BLOCK] * 2, args, f"upward{step}")
        args = [t0, y0, t1, y1, eta, inv, message] + others
        args += [] if first else [kept]
        body = functools.partial(implicit, first, last)
        if last:
            w_far, p_far = call(
                body,
                [BLOCK] * 2,
                args,
                f"implicit{step}",
                scratch=[vmem(*BLOCK), vmem(*BLOCK), pltpu.SemaphoreType.DMA((8,))],
                far_out=2,
                limit=3,
            )
        else:
            outs = [BLOCK, BLOCK, (2 * NI, NL), (2 * NK, NL), (2 * NK, NL), PACK]
            outs += [(sum(COUNTS) * NI, NL)] if first else []
            w, p, sums, to_up, to_down, own, *more = call(body, outs, args + [a_w, top_w], f"implicit{step}")
            to_right = to_left = own
            if first:
                kept = more[0]
    return tuple(x.reshape(NK, NI, NL) for x in (u_far, v_far, w_far, p_far))


def solution(mesh):
    return jax.shard_map(
        shards,
        mesh=mesh,
        in_specs=(P("lev", "gx", "gy"),) * 6,
        out_specs=(P("lev", "gx", "gy"),) * 4,
        check_vma=False,
    )
```

```python
import functools

import jax
import jax.numpy as jnp
from jax import lax
from jax.experimental import pallas as pl
from jax.experimental.pallas import tpu as pltpu
from jax.sharding import PartitionSpec as P

SUBSTEPS = 3

courant_h = 0.3
vertical_gain = 4096.0

F32 = jnp.float32
NI, NK, NL = 16, 64, 128

STEP = 24
PADDED = ((NK + 1) * STEP, NL)
BLOCK = (NI * NK, NL)
PACK = (4 * 8, NL)


def level(k):
    return pl.ds(NI * k, NI)


def row(i):
    return pl.ds(NK * i, NK)


def padded_row(i):
    return pl.ds(8 + i, NK, stride=STEP)


def main_rows(padded):
    return padded.reshape(NK + 1, STEP, NL).at[pl.ds(0, NK), pl.ds(8, NI), :]


def vmem(*shape):
    return pltpu.VMEM(shape, F32)


def hbm(*shape):
    return pltpu.HBM(shape, F32)


def call(body, outs, args, name, scratch=(), aliases=None, far_in=0, far_out=0, limit=2):
    near, far = pl.BlockSpec(memory_space=pltpu.VMEM), pl.BlockSpec(memory_space=pltpu.HBM)
    args = [
        pltpu.with_memory_space_constraint(x, pltpu.HBM if at < far_in else pltpu.VMEM) for at, x in enumerate(args)
    ]
    return pl.pallas_call(
        body,
        out_shape=tuple((hbm if at < far_out else vmem)(*shape) for at, shape in enumerate(outs)),
        in_specs=[far] * far_in + [near] * (len(args) - far_in),
        out_specs=(far,) * far_out + (near,) * (len(outs) - far_out),
        scratch_shapes=list(scratch),
        input_output_aliases=aliases or {},
        name=name,
        compiler_params=pltpu.CompilerParams(vmem_limit_bytes=limit << 20),
    )(*args)


def tiles():
    for group in range(4):
        for tile in range(32):
            yield group, tile, group * 16 + tile // 2, 8 * (tile % 2)


def pack_edges(load):
    lane = lax.broadcasted_iota(jnp.int32, (8, NL), 1) // 4
    packs = [jnp.zeros((8, NL), F32)] * 4
    for group, tile, k, i in tiles():
        rolled = pltpu.roll(load(k, i), 4 * tile + 2, 1)
        packs[group] = jnp.where(lane == tile, rolled, packs[group])
    return jnp.concatenate(packs, 0)


def slots(shape=PACK):
    return lax.broadcasted_iota(jnp.int32, shape, 1) % 4


def turn(x, by):
    return pltpu.roll(x, by % NL, 1)


def block_row(i):
    return pl.ds(i, NK, stride=NI)


def prologue(p_in, v_in, b_in, u_in, p, v, b, u, to_up, to_down, to_right, to_left, sems):
    copies = []
    for at, (source, target) in enumerate(((p_in, p), (v_in, v), (b_in, b), (u_in, u))):
        if at == 3:
            target = main_rows(target)
        copies.append(pltpu.make_async_copy(source, target, sems.at[at]))
    for copy in copies:
        copy.start()
    packs = []
    for copy, field in zip(copies, (p, v, b)):
        copy.wait()
        packs.append(pack_edges(lambda k, i: field[pl.ds(NI * k + i, 8), :]))
    edge_p, edge_v, edge_b = packs
    slot = slots()
    to_right[...] = jnp.where(slot < 2, edge_p, jnp.where(slot == 2, turn(edge_v, 1), turn(edge_b, 2)))
    to_left[...] = jnp.where(slot < 2, turn(edge_p, -2), jnp.where(slot == 2, edge_v, turn(edge_b, 1)))
    copies[3].wait()
    for at, (field, i) in enumerate(((p, 14), (p, 15), (u, 15), (b, 15))):
        to_up[row(at), :] = field[padded_row(i) if field is u else block_row(i), :]
    for at, (field, i) in enumerate(((p, 0), (p, 1), (u, 0), (b, 0))):
        to_down[row(at), :] = field[padded_row(i) if field is u else block_row(i), :]


def factor(
    s_in, w_in, b_in, v_in,
    theta, rest, g_out, eta, inv, t1, y1, a_p, top_p, a_w, top_w, v, b_v, statics, sums,
):
    first = s_in[level(0), :]
    passed = first
    held = None
    for k in range(NK):
        v[level(k), :] = turn(v_in[level(k), :], -1)
        b_v[level(k), :] = turn(b_in[level(k), :], -1)
        g = 1.0 / (vertical_gain * b_in[level(k), :])
        g_out[level(k), :] = g
        stiff = s_in[level(k), :]
        if k == 0:
            c = first
        else:
            ratio = 1.0 / (held + stiff)
            th = held * ratio
            rs = stiff * ratio
            theta[level(k), :] = th
            rest[level(k), :] = rs
            c = stiff * th
            passed = passed * rs
        held = g + c
        ic = 1.0 / held
        inv[level(k), :] = ic
        eta[level(k), :] = c * ic
        t1[level(k), :] = (g * ic) * passed
        y1[level(k), :] = passed * ic
    theta[level(0), :] = jnp.ones((NI, NL), F32)
    rest[level(0), :] = jnp.zeros((NI, NL), F32)
    statics[level(1), :] = passed
    statics[level(2), :] = held
    weight = jnp.ones((NI, NL), F32)
    above = jnp.zeros((NI, NL), F32)
    reply_above = None
    sum_a = jnp.zeros((NI, NL), F32)
    sum_t = jnp.zeros((NI, NL), F32)
    for k in range(NK - 1, -1, -1):
        g = g_out[level(k), :]
        w = w_in[level(k), :]
        top_p[level(k), :] = theta[level(k), :] * weight
        gw = g * weight
        top_w[level(k), :] = gw
        sum_t = sum_t + gw * w
        weight = weight * rest[level(k), :]
        reply = y1[level(k), :] - inv[level(k), :] * above
        above = t1[level(k), :] + eta[level(k), :] * above
        gr = g * reply
        a_w[level(k), :] = gr
        sum_a = sum_a - gr * w
        if reply_above is not None:
            a_p[level(k + 1), :] = reply - reply_above
        reply_above = reply
    a_p[level(0), :] = 1.0 - reply_above
    statics[level(0), :] = above
    sums[level(0), :] = sum_a
    sums[level(1), :] = sum_t


BATCH = 8
CHUNK = 8


def batches():
    for start in range(0, NK, BATCH):
        spots = range(2 * (start % 16), 2 * (start % 16) + 2 * BATCH)

        def spread(pack, by, spots=spots, group=slice(8 * (start // 16), 8 * (start // 16) + 8)):
            return jnp.concatenate([turn(pack[group, :], by - 4 * tile) for tile in spots], 0)

        yield start, pl.ds(NI * start, NI * BATCH), spread


def inner(first, p, u, v, b_u, b_v, s, u_new, v_part, star_part):
    for k in range(NK):
        rows = pl.ds(STEP * k + 8, NI)
        if k == 0:
            below = jnp.concatenate([p[pl.ds(0, 1), :], p[pl.ds(0, NI - 1), :]], 0)
        else:
            below = p[pl.ds(NI * k - 1, NI), :]
        if k == NK - 1:
            above = jnp.concatenate([p[pl.ds(NI * k + 1, NI - 1), :], p[pl.ds(NI * k, 1), :]], 0)
        else:
            above = p[pl.ds(NI * k + 1, NI), :]
        u_new[rows, :] = u[rows, :] - courant_h * b_u[level(k), :] * (above - below)
    lane = lax.broadcasted_iota(jnp.int32, (NI * BATCH, NL), 1)
    for _, rows, _ in batches():
        pressure = p[rows, :]
        p_next = jnp.where(lane >= NL - 2, 0.0, turn(pressure, -2))
        vn = v[rows, :] - courant_h * b_v[rows, :] * (p_next - pressure)
        if first:
            vn = jnp.where(lane == NL - 1, 0.0, vn)
        v_part[rows, :] = vn
        star_part[rows, :] = pressure - courant_h * s[rows, :] * (vn - jnp.where(lane < 2, 0.0, turn(vn, 2)))


def explicit(first, last, *refs):
    (p, u_old, b_u, star_part, s, a_p, top_p, sums, own, low, high, left, right, low0, high0, extra), refs = (
        refs[:16],
        refs[17:],
    )
    if first:
        own_right, refs = refs[0], refs[1:]
    else:
        u_sides, refs = refs[0], refs[1:]
    u, p_star, message, side = refs[:4]
    for n, (source, old) in enumerate(((low, low0), (high, high0))):
        away, edge, second = (1, 0, 1) if n == 0 else (-1, NI - 1, NI - 2)
        far, near = (0, 1) if n == 0 else (1, 0)
        held = old[row(2), :] if first else u_sides[row(n), :]
        held = held - courant_h * old[row(3), :] * (away * (p[block_row(edge), :] - source[row(far), :]))
        u[padded_row(edge - away), :] = held
        if not last:
            refs[4][row(n), :] = held
        u[padded_row(edge), :] = u_old[padded_row(edge), :] - courant_h * b_u[block_row(edge), :] * (
            away * (p[block_row(second), :] - source[row(near), :])
        )
    slot = slots()
    from_left = turn(left[...], 2)
    if first:
        mine, from_right = own[...], right[...]
        edge = turn(mine, 2)
        v_side = jnp.where(slot == 2, left[...], turn(mine, 1))
        b_pack = jnp.where(slot == 2, turn(left[...], -1), mine)
        b_edge = jnp.where(slot == 0, turn(own_right[...], -3), turn(from_right, -2))
        b_pack = jnp.where(slot < 2, b_edge, b_pack)
        ahead = turn(from_right, -1) - courant_h * b_edge * (from_right - own_right[...])
        taken = jnp.where(slot == 0, courant_h * b_edge * from_right, -ahead)
    else:
        edge = own[...]
        v_side, b_pack = extra[pl.ds(0, 32), :], extra[pl.ds(32, 32), :]
        taken = courant_h * b_pack * turn(right[...], -2)
    v_side = v_side - courant_h * b_pack * (edge - from_left)
    packed = jnp.where(slot < 2, taken, v_side)
    side[pl.ds(0, 32), :] = packed
    if not last:
        side[pl.ds(32, 32), :] = b_pack
    lane = lax.broadcasted_iota(jnp.int32, (NI * BATCH, NL), 1)
    at_edge = (lane < 2) | (lane >= NL - 2)
    total_a, total_t = sums[level(0), :], sums[level(1), :]
    for start, rows, spread in batches():
        du = jnp.concatenate(
            [
                u[pl.ds(STEP * k + 9, NI), :] - u[pl.ds(STEP * k + 7, NI), :]
                for k in range(start, start + BATCH)
            ],
            0,
        )
        star = star_part[rows, :] - courant_h * s[rows, :] * (du - jnp.where(at_edge, spread(packed, -2), 0.0))
        p_star[rows, :] = star
        part_a, part_t = a_p[rows, :] * star, top_p[rows, :] * star
        for k in range(BATCH):
            total_a = total_a + part_a[NI * k : NI * k + NI]
            total_t = total_t + part_t[NI * k : NI * k + NI]
    message[level(0), :] = total_a
    message[level(1), :] = total_t
    if first:
        message[pl.ds(2 * NI, 3 * NI), :] = extra[...]


def upward(first, last, *refs):
    (p_star, w, theta, rest, g_in, eta, inv, v_part, side), refs = refs[:9], refs[9:]
    copies = []
    if last:
        u, u_far, v_far, t0, y0, v_out, sems = refs

        def send(source, target):
            copies.append(pltpu.make_async_copy(source, target, sems.at[len(copies)]))
            copies[-1].start()

        send(main_rows(u), u_far)
    elif first:
        b_v, right, t0, y0, v_out, b_patched = refs
    else:
        t0, y0, v_out = refs
    lane = lax.broadcasted_iota(jnp.int32, (NI * BATCH, NL), 1)
    for _, rows, spread in batches():
        vn = v_part[rows, :] - jnp.where(lane >= NL - 2, spread(side, -2), 0.0)
        if last:
            vn = turn(jnp.where(lane == NL - 1, spread(side, -4), vn), 1)
        v_out[rows, :] = vn
        if last:
            send(v_out.at[rows, :], v_far.at[rows, :])
        if first:
            b_patched[rows, :] = jnp.where(lane == NL - 1, spread(right, NL - 4), b_v[rows, :])
    carried = held_gw = None
    for k in range(NK):
        star = p_star[level(k), :]
        gw = g_in[level(k), :] * w[level(k), :]
        if k == 0:
            carried = star
        else:
            carried = theta[level(k), :] * star + rest[level(k), :] * (carried + held_gw)
        held_gw = gw
        e = eta[level(k), :]
        t0[level(k), :] = carried - e * (carried + gw)
        y0[level(k), :] = (carried + gw) * inv[level(k), :]
    for copy in copies:
        copy.wait()


def interface(position, by_group, statics):
    a = [x[0:NI] for x in by_group]
    top = [x[NI : 2 * NI] for x in by_group]
    kappa, scale, shifted, reach, conduct = statics
    tops = [top[0]]
    for m in range(2):
        tops.append(scale[m] * top[m + 1] + shifted[m] * (tops[m] - a[m + 1]))
    y_above = jnp.zeros((NI, NL), F32)
    xs, ys = [None] * 3, [None] * 3
    for m in (2, 1, 0):
        xs[m] = kappa[m] * (tops[m] - a[m + 1] - (reach[m] * y_above if m < 2 else 0.0))
        ys[m] = tops[m] - conduct[m] * xs[m]
        y_above = ys[m]
    zero = jnp.zeros((NI, NL), F32)
    w_low = jnp.where(position == 0, zero, jnp.where(position == 1, xs[0], jnp.where(position == 2, xs[1], xs[2])))
    p_high = jnp.where(position == 3, zero, jnp.where(position == 2, ys[2], jnp.where(position == 1, ys[1], ys[0])))
    return w_low, p_high


def reduced_statics(by_group):
    beta = [x[2 * NI : 3 * NI] for x in by_group]
    phi = [x[3 * NI : 4 * NI] for x in by_group]
    grounded = [x[4 * NI : 5 * NI] for x in by_group]
    conduct = [grounded[0]]
    kappa, scale, shifted, reach = [], [], [], []
    for m in range(3):
        kappa.append(1.0 / (conduct[m] + beta[m + 1]))
        reach.append(phi[m + 1] / grounded[m + 1])
        if m < 2:
            coupled = phi[m + 1] * kappa[m]
            scale.append(1.0 / (1.0 + coupled * reach[m]))
            shifted.append(coupled * scale[m])
            conduct.append(grounded[m + 1] * scale[m])
    return kappa, scale, shifted, reach, conduct


COUNTS = (3, 2, 2, 3, 3)


def implicit(first, last, *refs):
    (t0, y0, t1, y1, eta, inv, own, by1, by2, by3), refs = refs[:10], refs[10:]
    if not first:
        kept, refs = refs[0], refs[1:]
    if last:
        w_far, p_far, w, p, sems = refs
    else:
        (a_w, top_w), (w, p, sums, to_up, to_down, edges), refs = refs[:2], refs[2:8], refs[8:]
    position = lax.axis_index("lev")
    others = [ref[...] for ref in (own, by1, by2, by3)]
    by_group = []
    for group in range(4):
        mask = position ^ group
        by_group.append(
            jnp.where(mask == 0, others[0], jnp.where(mask == 1, others[1], jnp.where(mask == 2, others[2], others[3])))
        )
    if first:
        statics = reduced_statics(by_group)
        keep, at = refs[0], 0
        for family in statics:
            for member in family:
                keep[level(at), :] = member
                at += 1
    else:
        statics, at = [], 0
        for count in COUNTS:
            statics.append([kept[level(at + m), :] for m in range(count)])
            at += count
    w_low, p_high = interface(position, by_group, statics)
    above = p_high
    sum_a = jnp.zeros((NI, NL), F32)
    sum_t = jnp.zeros((NI, NL), F32)
    copies = []
    for k in range(NK - 1, -1, -1):
        wn = y0[level(k), :] + y1[level(k), :] * w_low - inv[level(k), :] * above
        above = t0[level(k), :] + t1[level(k), :] * w_low + eta[level(k), :] * above
        w[level(k), :] = wn
        p[level(k), :] = above
        if last:
            if k % CHUNK == 0:
                part = pl.ds(NI * k, NI * CHUNK)
                for source, target in ((w, w_far), (p, p_far)):
                    copy = pltpu.make_async_copy(source.at[part, :], target.at[part, :], sems.at[len(copies)])
                    copy.start()
                    copies.append(copy)
        else:
            sum_a = sum_a - a_w[level(k), :] * wn
            sum_t = sum_t + top_w[level(k), :] * wn
    for copy in copies:
        copy.wait()
    if not last:
        sums[level(0), :] = sum_a
        sums[level(1), :] = sum_t
        for at, i in enumerate((14, 15)):
            to_up[row(at), :] = p[block_row(i), :]
        for at, i in enumerate((0, 1)):
            to_down[row(at), :] = p[block_row(i), :]
        edges[...] = pack_edges(lambda k, i: p[pl.ds(NI * k + i, 8), :])


def ring(block, axis, distance):
    size = lax.axis_size(axis)
    return lax.ppermute(block, axis, [(i, (i + distance) % size) for i in range(size)])


def partner(block, mask):
    return lax.ppermute(block, "lev", [(i, i ^ mask) for i in range(4)])


def shards(u_wind, v_wind, w_wind, pressure, buoyancy, stiffness):
    w, s = w_wind.reshape(BLOCK), stiffness.reshape(BLOCK)
    p, v, b, u, to_up, to_down, to_right, own = call(
        prologue,
        [BLOCK] * 3 + [PADDED, (4 * NK, NL), (4 * NK, NL), PACK, PACK],
        [x.reshape(BLOCK) for x in (pressure, v_wind, buoyancy)] + [u_wind],
        "prologue",
        scratch=[pltpu.SemaphoreType.DMA((4,))],
        far_in=4,
    )
    to_left = own
    (theta, rest, g, eta, inv, t1, y1, a_p, top_p, a_w, top_w, v, b_v, statics, sums) = call(
        factor, [BLOCK] * 13 + [(3 * NI, NL), (2 * NI, NL)], [s, w, b, v], "factor"
    )
    side, more = statics, [to_right]
    for step in range(SUBSTEPS):
        first, last = step == 0, step == SUBSTEPS - 1
        low, high = ring(to_up, "gx", 1), ring(to_down, "gx", -1)
        left, right = ring(to_right, "gy", 1), ring(to_left, "gy", -1)
        if first:
            gx_first = [low, high]
        u_part, v_part, star_part = call(
            functools.partial(inner, first), [PADDED, BLOCK, BLOCK], [p, u, v, b, b_v, s], f"inner{step}"
        )
        args = [p, u, b, star_part, s, a_p, top_p, sums, own, low, high, left, right] + gx_first + [side, u_part] + more
        outs = [PADDED, BLOCK, ((5 if first else 2) * NI, NL)]
        outs += [PACK] if last else [(2 * PACK[0], NL), (2 * NK, NL)]
        u, p_star, message, side, *more = call(
            functools.partial(explicit, first, last), outs, args, f"explicit{step}", aliases={16: 0}
        )
        others = [partner(message, mask) for mask in (1, 2, 3)]
        args = [p_star, w, theta, rest, g, eta, inv, v_part, side]
        outs = [BLOCK] * 3
        if last:
            u_far, v_far, t0, y0 = call(
                functools.partial(upward, False, True),
                [(NK, NI, NL)] + outs,
                args + [u],
                f"upward{step}",
                scratch=[vmem(*BLOCK), pltpu.SemaphoreType.DMA((1 + NK // BATCH,))],
                far_out=2,
            )
        elif first:
            t0, y0, v, b_v = call(
                functools.partial(upward, True, False), outs + [BLOCK], args + [b_v, right], f"upward{step}"
            )
        else:
            t0, y0, v = call(functools.partial(upward, False, False), outs, args, f"upward{step}")
        args = [t0, y0, t1, y1, eta, inv, message] + others
        args += [] if first else [kept]
        body = functools.partial(implicit, first, last)
        if last:
            w_far, p_far = call(
                body,
                [BLOCK] * 2,
                args,
                f"implicit{step}",
                scratch=[vmem(*BLOCK), vmem(*BLOCK), pltpu.SemaphoreType.DMA((2 * NK // CHUNK,))],
                far_out=2,
                limit=3,
            )
        else:
            outs = [BLOCK, BLOCK, (2 * NI, NL), (2 * NK, NL), (2 * NK, NL), PACK]
            outs += [(sum(COUNTS) * NI, NL)] if first else []
            w, p, sums, to_up, to_down, own, *fixed = call(body, outs, args + [a_w, top_w], f"implicit{step}")
            to_right = to_left = own
            if first:
                kept = fixed[0]
    return tuple(x.reshape(NK, NI, NL) for x in (u_far, v_far, w_far, p_far))


def solution(mesh):
    return jax.shard_map(
        shards,
        mesh=mesh,
        in_specs=(P("lev", "gx", "gy"),) * 6,
        out_specs=(P("lev", "gx", "gy"),) * 4,
        check_vma=False,
    )
```

```python
import functools

import jax
import jax.numpy as jnp
from jax import lax
from jax.experimental import pallas as pl
from jax.experimental.pallas import tpu as pltpu
from jax.sharding import PartitionSpec as P

SUBSTEPS = 3

courant_h = 0.3
vertical_gain = 4096.0

F32 = jnp.float32
NI, NK, NL = 16, 64, 128

STEP = 24
PADDED = ((NK + 1) * STEP, NL)
BLOCK = (NI * NK, NL)
PACK = (4 * 8, NL)


def level(k):
    return pl.ds(NI * k, NI)


def row(i):
    return pl.ds(NK * i, NK)


def padded_row(i):
    return pl.ds(8 + i, NK, stride=STEP)


def main_rows(padded):
    return padded.reshape(NK + 1, STEP, NL).at[pl.ds(0, NK), pl.ds(8, NI), :]


def vmem(*shape):
    return pltpu.VMEM(shape, F32)


def hbm(*shape):
    return pltpu.HBM(shape, F32)


def call(body, outs, args, name, scratch=(), aliases=None, far_in=0, far_out=0, limit=2):
    near, far = pl.BlockSpec(memory_space=pltpu.VMEM), pl.BlockSpec(memory_space=pltpu.HBM)
    args = [
        pltpu.with_memory_space_constraint(x, pltpu.HBM if at < far_in else pltpu.VMEM) for at, x in enumerate(args)
    ]
    return pl.pallas_call(
        body,
        out_shape=tuple((hbm if at < far_out else vmem)(*shape) for at, shape in enumerate(outs)),
        in_specs=[far] * far_in + [near] * (len(args) - far_in),
        out_specs=(far,) * far_out + (near,) * (len(outs) - far_out),
        scratch_shapes=list(scratch),
        input_output_aliases=aliases or {},
        name=name,
        compiler_params=pltpu.CompilerParams(vmem_limit_bytes=limit << 20),
    )(*args)


def tiles():
    for group in range(4):
        for tile in range(32):
            yield group, tile, group * 16 + tile // 2, 8 * (tile % 2)


def pack_edges(load):
    lane = lax.broadcasted_iota(jnp.int32, (8, NL), 1) // 4
    packs = [jnp.zeros((8, NL), F32)] * 4
    for group, tile, k, i in tiles():
        rolled = pltpu.roll(load(k, i), 4 * tile + 2, 1)
        packs[group] = jnp.where(lane == tile, rolled, packs[group])
    return jnp.concatenate(packs, 0)


def slots(shape=PACK):
    return lax.broadcasted_iota(jnp.int32, shape, 1) % 4


def turn(x, by):
    return pltpu.roll(x, by % NL, 1)


def block_row(i):
    return pl.ds(i, NK, stride=NI)


def is_even():
    return (lax.axis_index("gx") & 1) == 0


def prologue(p_in, v_in, b_in, u_in, p, v, b, u, to_chip, to_far, to_right, to_left, sems):
    copies = []
    for at, (source, target) in enumerate(((p_in, p), (v_in, v), (b_in, b), (u_in, u))):
        if at == 3:
            target = main_rows(target)
        copies.append(pltpu.make_async_copy(source, target, sems.at[at]))
    for copy in copies:
        copy.start()
    packs = []
    for copy, field in zip(copies, (p, v, b)):
        copy.wait()
        packs.append(pack_edges(lambda k, i: field[pl.ds(NI * k + i, 8), :]))
    edge_p, edge_v, edge_b = packs
    slot = slots()
    to_right[...] = jnp.where(slot < 2, edge_p, jnp.where(slot == 2, turn(edge_v, 1), turn(edge_b, 2)))
    to_left[...] = jnp.where(slot < 2, turn(edge_p, -2), jnp.where(slot == 2, edge_v, turn(edge_b, 1)))
    copies[3].wait()
    even = is_even()
    up, down = (
        [p[block_row(edge), :], u[padded_row(edge), :] + away * courant_h * b[block_row(edge), :] * p[block_row(next_to), :]]
        + [b[block_row(edge), :]]
        for edge, next_to, away in ((NI - 1, NI - 2, 1), (0, 1, -1))
    )
    for at in range(3):
        to_chip[row(at), :] = jnp.where(even, up[at], down[at])
        to_far[row(at), :] = jnp.where(even, down[at], up[at])


def factor(
    s_in, w_in, b_in, v_in,
    theta, rest, g_out, eta, inv, t1, y1, a_p, top_p, a_w, top_w, v, b_v, statics, sums,
):
    first = s_in[level(0), :]
    passed = first
    held = None
    for k in range(NK):
        v[level(k), :] = turn(v_in[level(k), :], -1)
        b_v[level(k), :] = turn(b_in[level(k), :], -1)
        g = 1.0 / (vertical_gain * b_in[level(k), :])
        g_out[level(k), :] = g
        stiff = s_in[level(k), :]
        if k == 0:
            c = first
        else:
            ratio = 1.0 / (held + stiff)
            th = held * ratio
            rs = stiff * ratio
            theta[level(k), :] = th
            rest[level(k), :] = rs
            c = stiff * th
            passed = passed * rs
        held = g + c
        ic = 1.0 / held
        inv[level(k), :] = ic
        eta[level(k), :] = c * ic
        t1[level(k), :] = (g * ic) * passed
        y1[level(k), :] = passed * ic
    theta[level(0), :] = jnp.ones((NI, NL), F32)
    rest[level(0), :] = jnp.zeros((NI, NL), F32)
    statics[level(1), :] = passed
    statics[level(2), :] = held
    weight = jnp.ones((NI, NL), F32)
    above = jnp.zeros((NI, NL), F32)
    reply_above = None
    sum_a = jnp.zeros((NI, NL), F32)
    sum_t = jnp.zeros((NI, NL), F32)
    for k in range(NK - 1, -1, -1):
        g = g_out[level(k), :]
        w = w_in[level(k), :]
        top_p[level(k), :] = theta[level(k), :] * weight
        gw = g * weight
        top_w[level(k), :] = gw
        sum_t = sum_t + gw * w
        weight = weight * rest[level(k), :]
        reply = y1[level(k), :] - inv[level(k), :] * above
        above = t1[level(k), :] + eta[level(k), :] * above
        gr = g * reply
        a_w[level(k), :] = gr
        sum_a = sum_a - gr * w
        if reply_above is not None:
            a_p[level(k + 1), :] = reply - reply_above
        reply_above = reply
    a_p[level(0), :] = 1.0 - reply_above
    statics[level(0), :] = above
    sums[level(0), :] = sum_a
    sums[level(1), :] = sum_t


BATCH = 8
CHUNK = 8


def batches():
    for start in range(0, NK, BATCH):
        spots = range(2 * (start % 16), 2 * (start % 16) + 2 * BATCH)

        def spread(pack, by, spots=spots, group=slice(8 * (start // 16), 8 * (start // 16) + 8)):
            return jnp.concatenate([turn(pack[group, :], by - 4 * tile) for tile in spots], 0)

        yield start, pl.ds(NI * start, NI * BATCH), spread


def inner(first, p, u, v, b_u, b_v, s, u_new, v_part, star_part):
    for k in range(NK):
        rows = pl.ds(STEP * k + 8, NI)
        if k == 0:
            below = jnp.concatenate([p[pl.ds(0, 1), :], p[pl.ds(0, NI - 1), :]], 0)
        else:
            below = p[pl.ds(NI * k - 1, NI), :]
        if k == NK - 1:
            above = jnp.concatenate([p[pl.ds(NI * k + 1, NI - 1), :], p[pl.ds(NI * k, 1), :]], 0)
        else:
            above = p[pl.ds(NI * k + 1, NI), :]
        u_new[rows, :] = u[rows, :] - courant_h * b_u[level(k), :] * (above - below)
    lane = lax.broadcasted_iota(jnp.int32, (NI * BATCH, NL), 1)
    for _, rows, _ in batches():
        pressure = p[rows, :]
        p_next = jnp.where(lane >= NL - 2, 0.0, turn(pressure, -2))
        vn = v[rows, :] - courant_h * b_v[rows, :] * (p_next - pressure)
        if first:
            vn = jnp.where(lane == NL - 1, 0.0, vn)
        v_part[rows, :] = vn
        star_part[rows, :] = pressure - courant_h * s[rows, :] * (vn - jnp.where(lane < 2, 0.0, turn(vn, 2)))


def explicit(first, last, *refs):
    (p, u_old, b_u, star_part, s, a_p, top_p, sums, own, chip, far, left, right, extra), refs = refs[:14], refs[15:]
    if first:
        own_right, refs = refs[0], refs[1:]
    else:
        u_sides, refs = refs[0], refs[1:]
    u, p_star, message, side = refs[:4]
    even = is_even()
    for n in (0, 1):
        away, edge, second = (1, 0, 1) if n == 0 else (-1, NI - 1, NI - 2)
        mine, other = (far, chip) if n == 0 else (chip, far)
        theirs = lambda at: jnp.where(even, mine[row(at), :], other[row(at), :])
        if first:
            near, held, b_side = theirs(0), theirs(1), theirs(2)
            held = held - away * courant_h * b_side * p[block_row(edge), :]
        else:
            near, b_side = theirs(0), u_sides[row(2 + n), :]
            held = u_sides[row(n), :] - away * courant_h * b_side * (p[block_row(edge), :] - theirs(1))
        u[padded_row(edge - away), :] = held
        if not last:
            refs[4][row(n), :] = held
            refs[4][row(2 + n), :] = b_side
        u[padded_row(edge), :] = u_old[padded_row(edge), :] - away * courant_h * b_u[block_row(edge), :] * (
            p[block_row(second), :] - near
        )
    slot = slots()
    from_left = turn(left[...], 2)
    if first:
        mine, from_right = own[...], right[...]
        edge = turn(mine, 2)
        v_side = jnp.where(slot == 2, left[...], turn(mine, 1))
        b_pack = jnp.where(slot == 2, turn(left[...], -1), mine)
        b_edge = jnp.where(slot == 0, turn(own_right[...], -3), turn(from_right, -2))
        b_pack = jnp.where(slot < 2, b_edge, b_pack)
        ahead = turn(from_right, -1) - courant_h * b_edge * (from_right - own_right[...])
        taken = jnp.where(slot == 0, courant_h * b_edge * from_right, -ahead)
    else:
        edge = own[...]
        v_side, b_pack = extra[pl.ds(0, 32), :], extra[pl.ds(32, 32), :]
        taken = courant_h * b_pack * turn(right[...], -2)
    v_side = v_side - courant_h * b_pack * (edge - from_left)
    packed = jnp.where(slot < 2, taken, v_side)
    side[pl.ds(0, 32), :] = packed
    if not last:
        side[pl.ds(32, 32), :] = b_pack
    lane = lax.broadcasted_iota(jnp.int32, (NI * BATCH, NL), 1)
    at_edge = (lane < 2) | (lane >= NL - 2)
    total_a, total_t = sums[level(0), :], sums[level(1), :]
    for start, rows, spread in batches():
        du = jnp.concatenate(
            [
                u[pl.ds(STEP * k + 9, NI), :] - u[pl.ds(STEP * k + 7, NI), :]
                for k in range(start, start + BATCH)
            ],
            0,
        )
        star = star_part[rows, :] - courant_h * s[rows, :] * (du - jnp.where(at_edge, spread(packed, -2), 0.0))
        p_star[rows, :] = star
        part_a, part_t = a_p[rows, :] * star, top_p[rows, :] * star
        for k in range(BATCH):
            total_a = total_a + part_a[NI * k : NI * k + NI]
            total_t = total_t + part_t[NI * k : NI * k + NI]
    message[level(0), :] = total_a
    message[level(1), :] = total_t
    if first:
        message[pl.ds(2 * NI, 3 * NI), :] = extra[...]


def upward(first, last, *refs):
    (p_star, w, theta, rest, g_in, eta, inv, v_part, side), refs = refs[:9], refs[9:]
    copies = []
    if last:
        u, u_far, v_far, t0, y0, v_out, sems = refs

        def send(source, target):
            copies.append(pltpu.make_async_copy(source, target, sems.at[len(copies)]))
            copies[-1].start()

        send(main_rows(u), u_far)
    elif first:
        b_v, right, t0, y0, v_out, b_patched = refs
    else:
        t0, y0, v_out = refs
    lane = lax.broadcasted_iota(jnp.int32, (NI * BATCH, NL), 1)
    for _, rows, spread in batches():
        vn = v_part[rows, :] - jnp.where(lane >= NL - 2, spread(side, -2), 0.0)
        if last:
            vn = turn(jnp.where(lane == NL - 1, spread(side, -4), vn), 1)
        v_out[rows, :] = vn
        if last:
            send(v_out.at[rows, :], v_far.at[rows, :])
        if first:
            b_patched[rows, :] = jnp.where(lane == NL - 1, spread(right, NL - 4), b_v[rows, :])
    carried = held_gw = None
    for k in range(NK):
        star = p_star[level(k), :]
        gw = g_in[level(k), :] * w[level(k), :]
        if k == 0:
            carried = star
        else:
            carried = theta[level(k), :] * star + rest[level(k), :] * (carried + held_gw)
        held_gw = gw
        e = eta[level(k), :]
        t0[level(k), :] = carried - e * (carried + gw)
        y0[level(k), :] = (carried + gw) * inv[level(k), :]
    for copy in copies:
        copy.wait()


def interface(position, by_group, statics):
    a = [x[0:NI] for x in by_group]
    top = [x[NI : 2 * NI] for x in by_group]
    kappa, scale, shifted, reach, conduct = statics
    tops = [top[0]]
    for m in range(2):
        tops.append(scale[m] * top[m + 1] + shifted[m] * (tops[m] - a[m + 1]))
    y_above = jnp.zeros((NI, NL), F32)
    xs, ys = [None] * 3, [None] * 3
    for m in (2, 1, 0):
        xs[m] = kappa[m] * (tops[m] - a[m + 1] - (reach[m] * y_above if m < 2 else 0.0))
        ys[m] = tops[m] - conduct[m] * xs[m]
        y_above = ys[m]
    zero = jnp.zeros((NI, NL), F32)
    w_low = jnp.where(position == 0, zero, jnp.where(position == 1, xs[0], jnp.where(position == 2, xs[1], xs[2])))
    p_high = jnp.where(position == 3, zero, jnp.where(position == 2, ys[2], jnp.where(position == 1, ys[1], ys[0])))
    return w_low, p_high


def reduced_statics(by_group):
    beta = [x[2 * NI : 3 * NI] for x in by_group]
    phi = [x[3 * NI : 4 * NI] for x in by_group]
    grounded = [x[4 * NI : 5 * NI] for x in by_group]
    conduct = [grounded[0]]
    kappa, scale, shifted, reach = [], [], [], []
    for m in range(3):
        kappa.append(1.0 / (conduct[m] + beta[m + 1]))
        reach.append(phi[m + 1] / grounded[m + 1])
        if m < 2:
            coupled = phi[m + 1] * kappa[m]
            scale.append(1.0 / (1.0 + coupled * reach[m]))
            shifted.append(coupled * scale[m])
            conduct.append(grounded[m + 1] * scale[m])
    return kappa, scale, shifted, reach, conduct


COUNTS = (3, 2, 2, 3, 3)


def implicit(first, last, *refs):
    (t0, y0, t1, y1, eta, inv, own, by1, by2, by3), refs = refs[:10], refs[10:]
    if not first:
        kept, refs = refs[0], refs[1:]
    if last:
        w_far, p_far, w, p, sems = refs
    else:
        (a_w, top_w), (w, p, sums, to_chip, to_far, edges), refs = refs[:2], refs[2:8], refs[8:]
    position = lax.axis_index("lev")
    others = [ref[...] for ref in (own, by1, by2, by3)]
    by_group = []
    for group in range(4):
        mask = position ^ group
        by_group.append(
            jnp.where(mask == 0, others[0], jnp.where(mask == 1, others[1], jnp.where(mask == 2, others[2], others[3])))
        )
    if first:
        statics = reduced_statics(by_group)
        keep, at = refs[0], 0
        for family in statics:
            for member in family:
                keep[level(at), :] = member
                at += 1
    else:
        statics, at = [], 0
        for count in COUNTS:
            statics.append([kept[level(at + m), :] for m in range(count)])
            at += count
    w_low, p_high = interface(position, by_group, statics)
    above = p_high
    sum_a = jnp.zeros((NI, NL), F32)
    sum_t = jnp.zeros((NI, NL), F32)
    copies = []
    for k in range(NK - 1, -1, -1):
        wn = y0[level(k), :] + y1[level(k), :] * w_low - inv[level(k), :] * above
        above = t0[level(k), :] + t1[level(k), :] * w_low + eta[level(k), :] * above
        w[level(k), :] = wn
        p[level(k), :] = above
        if last:
            if k % CHUNK == 0:
                part = pl.ds(NI * k, NI * CHUNK)
                for source, target in ((w, w_far), (p, p_far)):
                    copy = pltpu.make_async_copy(source.at[part, :], target.at[part, :], sems.at[len(copies)])
                    copy.start()
                    copies.append(copy)
        else:
            sum_a = sum_a - a_w[level(k), :] * wn
            sum_t = sum_t + top_w[level(k), :] * wn
    for copy in copies:
        copy.wait()
    if not last:
        sums[level(0), :] = sum_a
        sums[level(1), :] = sum_t
        even = is_even()
        for at, (i, j) in enumerate(((NI - 1, 0), (NI - 2, 1))):
            up, down = p[block_row(i), :], p[block_row(j), :]
            to_chip[row(at), :] = jnp.where(even, up, down)
            to_far[row(at), :] = jnp.where(even, down, up)
        edges[...] = pack_edges(lambda k, i: p[pl.ds(NI * k + i, 8), :])


def ring(block, axis, distance):
    size = lax.axis_size(axis)
    return lax.ppermute(block, axis, [(i, (i + distance) % size) for i in range(size)])


def swap(block, first):
    size = lax.axis_size("gx")
    pairs = [(i, (i + 1) % size) for i in range(first, size, 2)]
    return lax.ppermute(block, "gx", pairs + [(j, i) for i, j in pairs])


def partner(block, mask):
    return lax.ppermute(block, "lev", [(i, i ^ mask) for i in range(4)])


def shards(u_wind, v_wind, w_wind, pressure, buoyancy, stiffness):
    w, s = w_wind.reshape(BLOCK), stiffness.reshape(BLOCK)
    p, v, b, u, to_chip, to_far, to_right, own = call(
        prologue,
        [BLOCK] * 3 + [PADDED, (3 * NK, NL), (3 * NK, NL), PACK, PACK],
        [x.reshape(BLOCK) for x in (pressure, v_wind, buoyancy)] + [u_wind],
        "prologue",
        scratch=[pltpu.SemaphoreType.DMA((4,))],
        far_in=4,
    )
    to_left = own
    (theta, rest, g, eta, inv, t1, y1, a_p, top_p, a_w, top_w, v, b_v, statics, sums) = call(
        factor, [BLOCK] * 13 + [(3 * NI, NL), (2 * NI, NL)], [s, w, b, v], "factor"
    )
    side, more = statics, [to_right]
    for step in range(SUBSTEPS):
        first, last = step == 0, step == SUBSTEPS - 1
        chip, far = swap(to_chip, 0), swap(to_far, 1)
        left, right = ring(to_right, "gy", 1), ring(to_left, "gy", -1)
        u_part, v_part, star_part = call(
            functools.partial(inner, first), [PADDED, BLOCK, BLOCK], [p, u, v, b, b_v, s], f"inner{step}"
        )
        args = [p, u, b, star_part, s, a_p, top_p, sums, own, chip, far, left, right, side, u_part] + more
        outs = [PADDED, BLOCK, ((5 if first else 2) * NI, NL)]
        outs += [PACK] if last else [(2 * PACK[0], NL), (4 * NK, NL)]
        u, p_star, message, side, *more = call(
            functools.partial(explicit, first, last), outs, args, f"explicit{step}", aliases={14: 0}
        )
        by1, by3, by2 = (partner(message, mask) for mask in (1, 3, 2))
        args = [p_star, w, theta, rest, g, eta, inv, v_part, side]
        outs = [BLOCK] * 3
        if last:
            u_far, v_far, t0, y0 = call(
                functools.partial(upward, False, True),
                [(NK, NI, NL)] + outs,
                args + [u],
                f"upward{step}",
                scratch=[vmem(*BLOCK), pltpu.SemaphoreType.DMA((1 + NK // BATCH,))],
                far_out=2,
            )
        elif first:
            t0, y0, v, b_v = call(
                functools.partial(upward, True, False), outs + [BLOCK], args + [b_v, right], f"upward{step}"
            )
        else:
            t0, y0, v = call(functools.partial(upward, False, False), outs, args, f"upward{step}")
        args = [t0, y0, t1, y1, eta, inv, message, by1, by2, by3]
        args += [] if first else [kept]
        body = functools.partial(implicit, first, last)
        if last:
            w_far, p_far = call(
                body,
                [BLOCK] * 2,
                args,
                f"implicit{step}",
                scratch=[vmem(*BLOCK), vmem(*BLOCK), pltpu.SemaphoreType.DMA((2 * NK // CHUNK,))],
                far_out=2,
                limit=3,
            )
        else:
            outs = [BLOCK, BLOCK, (2 * NI, NL), (2 * NK, NL), (2 * NK, NL), PACK]
            outs += [(sum(COUNTS) * NI, NL)] if first else []
            w, p, sums, to_chip, to_far, own, *fixed = call(body, outs, args + [a_w, top_w], f"implicit{step}")
            to_right = to_left = own
            if first:
                kept = fixed[0]
    return tuple(x.reshape(NK, NI, NL) for x in (u_far, v_far, w_far, p_far))


def solution(mesh):
    return jax.shard_map(
        shards,
        mesh=mesh,
        in_specs=(P("lev", "gx", "gy"),) * 6,
        out_specs=(P("lev", "gx", "gy"),) * 4,
        check_vma=False,
    )
```

```python
import functools

import jax
import jax.numpy as jnp
from jax import lax
from jax.experimental import pallas as pl
from jax.experimental.pallas import tpu as pltpu
from jax.sharding import PartitionSpec as P

SUBSTEPS = 3

courant_h = 0.3
vertical_gain = 4096.0

F32 = jnp.float32
NI, NK, NL = 16, 64, 128

STEP = 24
PADDED = ((NK + 1) * STEP, NL)
BLOCK = (NI * NK, NL)
PACK = (4 * 8, NL)


def level(k):
    return pl.ds(NI * k, NI)


def row(i):
    return pl.ds(NK * i, NK)


def padded_row(i):
    return pl.ds(8 + i, NK, stride=STEP)


def main_rows(padded):
    return padded.reshape(NK + 1, STEP, NL).at[pl.ds(0, NK), pl.ds(8, NI), :]


def vmem(*shape):
    return pltpu.VMEM(shape, F32)


def hbm(*shape):
    return pltpu.HBM(shape, F32)


def call(body, outs, args, name, scratch=(), aliases=None, far_in=0, far_out=0, limit=2):
    near, far = pl.BlockSpec(memory_space=pltpu.VMEM), pl.BlockSpec(memory_space=pltpu.HBM)
    args = [
        pltpu.with_memory_space_constraint(x, pltpu.HBM if at < far_in else pltpu.VMEM) for at, x in enumerate(args)
    ]
    return pl.pallas_call(
        body,
        out_shape=tuple((hbm if at < far_out else vmem)(*shape) for at, shape in enumerate(outs)),
        in_specs=[far] * far_in + [near] * (len(args) - far_in),
        out_specs=(far,) * far_out + (near,) * (len(outs) - far_out),
        scratch_shapes=list(scratch),
        input_output_aliases=aliases or {},
        name=name,
        compiler_params=pltpu.CompilerParams(vmem_limit_bytes=limit << 20),
    )(*args)


def tiles():
    for group in range(4):
        for tile in range(32):
            yield group, tile, group * 16 + tile // 2, 8 * (tile % 2)


def pack_edges(load):
    lane = lax.broadcasted_iota(jnp.int32, (8, NL), 1) // 4
    packs = [jnp.zeros((8, NL), F32)] * 4
    for group, tile, k, i in tiles():
        rolled = pltpu.roll(load(k, i), 4 * tile + 2, 1)
        packs[group] = jnp.where(lane == tile, rolled, packs[group])
    return jnp.concatenate(packs, 0)


def slots(shape=PACK):
    return lax.broadcasted_iota(jnp.int32, shape, 1) % 4


def turn(x, by):
    return pltpu.roll(x, by % NL, 1)


def block_row(i):
    return pl.ds(i, NK, stride=NI)


def is_even(axis):
    return (lax.axis_index(axis) & 1) == 0


def prologue(p_in, v_in, b_in, u_in, p, v, b, u, to_chip, to_far, to_right, to_left, to_first, to_second, sems):
    copies = []
    for at, (source, target) in enumerate(((p_in, p), (v_in, v), (b_in, b), (u_in, u))):
        if at == 3:
            target = main_rows(target)
        copies.append(pltpu.make_async_copy(source, target, sems.at[at]))
    for copy in copies:
        copy.start()
    packs = []
    for copy, field in zip(copies, (p, v, b)):
        copy.wait()
        packs.append(pack_edges(lambda k, i: field[pl.ds(NI * k + i, 8), :]))
    edge_p, edge_v, edge_b = packs
    slot = slots()
    going_right = jnp.where(slot < 2, edge_p, jnp.where(slot == 2, turn(edge_v, 1), turn(edge_b, 2)))
    going_left = jnp.where(slot < 2, turn(edge_p, -2), jnp.where(slot == 2, edge_v, turn(edge_b, 1)))
    to_right[...] = going_right
    to_left[...] = going_left
    even = is_even("gy")
    to_first[...] = jnp.where(even, going_right, going_left)
    to_second[...] = jnp.where(even, going_left, going_right)
    copies[3].wait()
    even = is_even("gx")
    up, down = (
        [p[block_row(edge), :], u[padded_row(edge), :] + away * courant_h * b[block_row(edge), :] * p[block_row(next_to), :]]
        + [b[block_row(edge), :]]
        for edge, next_to, away in ((NI - 1, NI - 2, 1), (0, 1, -1))
    )
    for at in range(3):
        to_chip[row(at), :] = jnp.where(even, up[at], down[at])
        to_far[row(at), :] = jnp.where(even, down[at], up[at])


def factor(
    s_in, w_in, b_in, v_in,
    theta, rest, g_out, eta, inv, t1, y1, a_p, top_p, a_w, top_w, v, b_v, statics, sums,
):
    first = s_in[level(0), :]
    passed = first
    held = None
    for k in range(NK):
        v[level(k), :] = turn(v_in[level(k), :], -1)
        b_v[level(k), :] = turn(b_in[level(k), :], -1)
        g = 1.0 / (vertical_gain * b_in[level(k), :])
        g_out[level(k), :] = g
        stiff = s_in[level(k), :]
        if k == 0:
            c = first
        else:
            ratio = 1.0 / (held + stiff)
            th = held * ratio
            rs = stiff * ratio
            theta[level(k), :] = th
            rest[level(k), :] = rs
            c = stiff * th
            passed = passed * rs
        held = g + c
        ic = 1.0 / held
        inv[level(k), :] = ic
        eta[level(k), :] = c * ic
        t1[level(k), :] = (g * ic) * passed
        y1[level(k), :] = passed * ic
    theta[level(0), :] = jnp.ones((NI, NL), F32)
    rest[level(0), :] = jnp.zeros((NI, NL), F32)
    statics[level(1), :] = passed
    statics[level(2), :] = held
    weight = jnp.ones((NI, NL), F32)
    above = jnp.zeros((NI, NL), F32)
    reply_above = None
    sum_a = jnp.zeros((NI, NL), F32)
    sum_t = jnp.zeros((NI, NL), F32)
    for k in range(NK - 1, -1, -1):
        g = g_out[level(k), :]
        w = w_in[level(k), :]
        top_p[level(k), :] = theta[level(k), :] * weight
        gw = g * weight
        top_w[level(k), :] = gw
        sum_t = sum_t + gw * w
        weight = weight * rest[level(k), :]
        reply = y1[level(k), :] - inv[level(k), :] * above
        above = t1[level(k), :] + eta[level(k), :] * above
        gr = g * reply
        a_w[level(k), :] = gr
        sum_a = sum_a - gr * w
        if reply_above is not None:
            a_p[level(k + 1), :] = reply - reply_above
        reply_above = reply
    a_p[level(0), :] = 1.0 - reply_above
    statics[level(0), :] = above
    sums[level(0), :] = sum_a
    sums[level(1), :] = sum_t


BATCH = 8
CHUNK = 8


def batches():
    for start in range(0, NK, BATCH):
        spots = range(2 * (start % 16), 2 * (start % 16) + 2 * BATCH)

        def spread(pack, by, spots=spots, group=slice(8 * (start // 16), 8 * (start // 16) + 8)):
            return jnp.concatenate([turn(pack[group, :], by - 4 * tile) for tile in spots], 0)

        yield start, pl.ds(NI * start, NI * BATCH), spread


def inner(first, p, u, v, b_u, b_v, s, u_new, v_part, star_part):
    for k in range(NK):
        rows = pl.ds(STEP * k + 8, NI)
        if k == 0:
            below = jnp.concatenate([p[pl.ds(0, 1), :], p[pl.ds(0, NI - 1), :]], 0)
        else:
            below = p[pl.ds(NI * k - 1, NI), :]
        if k == NK - 1:
            above = jnp.concatenate([p[pl.ds(NI * k + 1, NI - 1), :], p[pl.ds(NI * k, 1), :]], 0)
        else:
            above = p[pl.ds(NI * k + 1, NI), :]
        u_new[rows, :] = u[rows, :] - courant_h * b_u[level(k), :] * (above - below)
    lane = lax.broadcasted_iota(jnp.int32, (NI * BATCH, NL), 1)
    for _, rows, _ in batches():
        pressure = p[rows, :]
        p_next = jnp.where(lane >= NL - 2, 0.0, turn(pressure, -2))
        vn = v[rows, :] - courant_h * b_v[rows, :] * (p_next - pressure)
        if first:
            vn = jnp.where(lane == NL - 1, 0.0, vn)
        v_part[rows, :] = vn
        star_part[rows, :] = pressure - courant_h * s[rows, :] * (vn - jnp.where(lane < 2, 0.0, turn(vn, 2)))


def explicit(first, last, *refs):
    (p, u_old, b_u, star_part, s, a_p, top_p, sums, own, chip, far, by_first, by_second, extra), refs = refs[:14], refs[15:]
    if first:
        own_right, refs = refs[0], refs[1:]
    else:
        u_sides, refs = refs[0], refs[1:]
    u, p_star, message, side = refs[:4]
    even = is_even("gx")
    for n in (0, 1):
        away, edge, second = (1, 0, 1) if n == 0 else (-1, NI - 1, NI - 2)
        mine, other = (far, chip) if n == 0 else (chip, far)
        theirs = lambda at: jnp.where(even, mine[row(at), :], other[row(at), :])
        if first:
            near, held, b_side = theirs(0), theirs(1), theirs(2)
            held = held - away * courant_h * b_side * p[block_row(edge), :]
        else:
            near, b_side = theirs(0), u_sides[row(2 + n), :]
            held = u_sides[row(n), :] - away * courant_h * b_side * (p[block_row(edge), :] - theirs(1))
        u[padded_row(edge - away), :] = held
        if not last:
            refs[4][row(n), :] = held
            refs[4][row(2 + n), :] = b_side
        u[padded_row(edge), :] = u_old[padded_row(edge), :] - away * courant_h * b_u[block_row(edge), :] * (
            p[block_row(second), :] - near
        )
    slot = slots()
    even = is_even("gy")
    left = jnp.where(even, by_second[...], by_first[...])
    right = jnp.where(even, by_first[...], by_second[...])
    from_left = turn(left, 2)
    if first:
        mine, from_right = own[...], right
        edge = turn(mine, 2)
        v_side = jnp.where(slot == 2, left, turn(mine, 1))
        b_pack = jnp.where(slot == 2, turn(left, -1), mine)
        b_edge = jnp.where(slot == 0, turn(own_right[...], -3), turn(from_right, -2))
        b_pack = jnp.where(slot < 2, b_edge, b_pack)
        ahead = turn(from_right, -1) - courant_h * b_edge * (from_right - own_right[...])
        taken = jnp.where(slot == 0, courant_h * b_edge * from_right, -ahead)
    else:
        edge = own[...]
        v_side, b_pack = extra[pl.ds(0, 32), :], extra[pl.ds(32, 32), :]
        taken = courant_h * b_pack * turn(right, -2)
    v_side = v_side - courant_h * b_pack * (edge - from_left)
    packed = jnp.where(slot < 2, taken, v_side)
    side[pl.ds(0, 32), :] = packed
    if not last:
        side[pl.ds(32, 32), :] = b_pack
    lane = lax.broadcasted_iota(jnp.int32, (NI * BATCH, NL), 1)
    at_edge = (lane < 2) | (lane >= NL - 2)
    total_a, total_t = sums[level(0), :], sums[level(1), :]
    for start, rows, spread in batches():
        du = jnp.concatenate(
            [
                u[pl.ds(STEP * k + 9, NI), :] - u[pl.ds(STEP * k + 7, NI), :]
                for k in range(start, start + BATCH)
            ],
            0,
        )
        star = star_part[rows, :] - courant_h * s[rows, :] * (du - jnp.where(at_edge, spread(packed, -2), 0.0))
        p_star[rows, :] = star
        part_a, part_t = a_p[rows, :] * star, top_p[rows, :] * star
        for k in range(BATCH):
            total_a = total_a + part_a[NI * k : NI * k + NI]
            total_t = total_t + part_t[NI * k : NI * k + NI]
    message[level(0), :] = total_a
    message[level(1), :] = total_t
    if first:
        message[pl.ds(2 * NI, 3 * NI), :] = extra[...]


def upward(first, last, *refs):
    (p_star, w, theta, rest, g_in, eta, inv, v_part, side), refs = refs[:9], refs[9:]
    copies = []
    if last:
        u, u_far, v_far, t0, y0, v_out, sems = refs

        def send(source, target):
            copies.append(pltpu.make_async_copy(source, target, sems.at[len(copies)]))
            copies[-1].start()

        send(main_rows(u), u_far)
    elif first:
        b_v, by_first, by_second, t0, y0, v_out, b_patched = refs
        right = jnp.where(is_even("gy"), by_first[...], by_second[...])
    else:
        t0, y0, v_out = refs
    lane = lax.broadcasted_iota(jnp.int32, (NI * BATCH, NL), 1)
    for _, rows, spread in batches():
        vn = v_part[rows, :] - jnp.where(lane >= NL - 2, spread(side, -2), 0.0)
        if last:
            vn = turn(jnp.where(lane == NL - 1, spread(side, -4), vn), 1)
        v_out[rows, :] = vn
        if last:
            send(v_out.at[rows, :], v_far.at[rows, :])
        if first:
            b_patched[rows, :] = jnp.where(lane == NL - 1, spread(right, NL - 4), b_v[rows, :])
    carried = held_gw = None
    for k in range(NK):
        star = p_star[level(k), :]
        gw = g_in[level(k), :] * w[level(k), :]
        if k == 0:
            carried = star
        else:
            carried = theta[level(k), :] * star + rest[level(k), :] * (carried + held_gw)
        held_gw = gw
        e = eta[level(k), :]
        t0[level(k), :] = carried - e * (carried + gw)
        y0[level(k), :] = (carried + gw) * inv[level(k), :]
    for copy in copies:
        copy.wait()


def interface(position, by_group, statics):
    a = [x[0:NI] for x in by_group]
    top = [x[NI : 2 * NI] for x in by_group]
    kappa, scale, shifted, reach, conduct = statics
    tops = [top[0]]
    for m in range(2):
        tops.append(scale[m] * top[m + 1] + shifted[m] * (tops[m] - a[m + 1]))
    y_above = jnp.zeros((NI, NL), F32)
    xs, ys = [None] * 3, [None] * 3
    for m in (2, 1, 0):
        xs[m] = kappa[m] * (tops[m] - a[m + 1] - (reach[m] * y_above if m < 2 else 0.0))
        ys[m] = tops[m] - conduct[m] * xs[m]
        y_above = ys[m]
    zero = jnp.zeros((NI, NL), F32)
    w_low = jnp.where(position == 0, zero, jnp.where(position == 1, xs[0], jnp.where(position == 2, xs[1], xs[2])))
    p_high = jnp.where(position == 3, zero, jnp.where(position == 2, ys[2], jnp.where(position == 1, ys[1], ys[0])))
    return w_low, p_high


def reduced_statics(by_group):
    beta = [x[2 * NI : 3 * NI] for x in by_group]
    phi = [x[3 * NI : 4 * NI] for x in by_group]
    grounded = [x[4 * NI : 5 * NI] for x in by_group]
    conduct = [grounded[0]]
    kappa, scale, shifted, reach = [], [], [], []
    for m in range(3):
        kappa.append(1.0 / (conduct[m] + beta[m + 1]))
        reach.append(phi[m + 1] / grounded[m + 1])
        if m < 2:
            coupled = phi[m + 1] * kappa[m]
            scale.append(1.0 / (1.0 + coupled * reach[m]))
            shifted.append(coupled * scale[m])
            conduct.append(grounded[m + 1] * scale[m])
    return kappa, scale, shifted, reach, conduct


COUNTS = (3, 2, 2, 3, 3)


def implicit(first, last, *refs):
    (t0, y0, t1, y1, eta, inv, own, by1, by2, by3), refs = refs[:10], refs[10:]
    if not first:
        kept, refs = refs[0], refs[1:]
    if last:
        w_far, p_far, w, p, sems = refs
    else:
        (a_w, top_w), (w, p, sums, to_chip, to_far, edges), refs = refs[:2], refs[2:8], refs[8:]
    position = lax.axis_index("lev")
    others = [ref[...] for ref in (own, by1, by2, by3)]
    by_group = []
    for group in range(4):
        mask = position ^ group
        by_group.append(
            jnp.where(mask == 0, others[0], jnp.where(mask == 1, others[1], jnp.where(mask == 2, others[2], others[3])))
        )
    if first:
        statics = reduced_statics(by_group)
        keep, at = refs[0], 0
        for family in statics:
            for member in family:
                keep[level(at), :] = member
                at += 1
    else:
        statics, at = [], 0
        for count in COUNTS:
            statics.append([kept[level(at + m), :] for m in range(count)])
            at += count
    w_low, p_high = interface(position, by_group, statics)
    above = p_high
    sum_a = jnp.zeros((NI, NL), F32)
    sum_t = jnp.zeros((NI, NL), F32)
    copies = []
    for k in range(NK - 1, -1, -1):
        wn = y0[level(k), :] + y1[level(k), :] * w_low - inv[level(k), :] * above
        above = t0[level(k), :] + t1[level(k), :] * w_low + eta[level(k), :] * above
        w[level(k), :] = wn
        p[level(k), :] = above
        if last:
            if k % CHUNK == 0:
                part = pl.ds(NI * k, NI * CHUNK)
                for source, target in ((w, w_far), (p, p_far)):
                    copy = pltpu.make_async_copy(source.at[part, :], target.at[part, :], sems.at[len(copies)])
                    copy.start()
                    copies.append(copy)
        else:
            sum_a = sum_a - a_w[level(k), :] * wn
            sum_t = sum_t + top_w[level(k), :] * wn
    for copy in copies:
        copy.wait()
    if not last:
        sums[level(0), :] = sum_a
        sums[level(1), :] = sum_t
        even = is_even("gx")
        for at, (i, j) in enumerate(((NI - 1, 0), (NI - 2, 1))):
            up, down = p[block_row(i), :], p[block_row(j), :]
            to_chip[row(at), :] = jnp.where(even, up, down)
            to_far[row(at), :] = jnp.where(even, down, up)
        edges[...] = pack_edges(lambda k, i: p[pl.ds(NI * k + i, 8), :])


def swap(block, axis, first):
    size = lax.axis_size(axis)
    pairs = [(i, (i + 1) % size) for i in range(first, size, 2)]
    return lax.ppermute(block, axis, pairs + [(j, i) for i, j in pairs])


def partner(block, mask):
    return lax.ppermute(block, "lev", [(i, i ^ mask) for i in range(4)])


def shards(u_wind, v_wind, w_wind, pressure, buoyancy, stiffness):
    w, s = w_wind.reshape(BLOCK), stiffness.reshape(BLOCK)
    p, v, b, u, to_chip, to_far, to_right, own, to_first, to_second = call(
        prologue,
        [BLOCK] * 3 + [PADDED, (3 * NK, NL), (3 * NK, NL)] + [PACK] * 4,
        [x.reshape(BLOCK) for x in (pressure, v_wind, buoyancy)] + [u_wind],
        "prologue",
        scratch=[pltpu.SemaphoreType.DMA((4,))],
        far_in=4,
    )
    (theta, rest, g, eta, inv, t1, y1, a_p, top_p, a_w, top_w, v, b_v, statics, sums) = call(
        factor, [BLOCK] * 13 + [(3 * NI, NL), (2 * NI, NL)], [s, w, b, v], "factor"
    )
    side, more = statics, [to_right]
    for step in range(SUBSTEPS):
        first, last = step == 0, step == SUBSTEPS - 1
        chip, far = swap(to_chip, "gx", 0), swap(to_far, "gx", 1)
        by_first, by_second = swap(to_first, "gy", 0), swap(to_second, "gy", 1)
        u_part, v_part, star_part = call(
            functools.partial(inner, first), [PADDED, BLOCK, BLOCK], [p, u, v, b, b_v, s], f"inner{step}"
        )
        args = [p, u, b, star_part, s, a_p, top_p, sums, own, chip, far, by_first, by_second, side, u_part] + more
        outs = [PADDED, BLOCK, ((5 if first else 2) * NI, NL)]
        outs += [PACK] if last else [(2 * PACK[0], NL), (4 * NK, NL)]
        u, p_star, message, side, *more = call(
            functools.partial(explicit, first, last), outs, args, f"explicit{step}", aliases={14: 0}
        )
        by1, by3, by2 = (partner(message, mask) for mask in (1, 3, 2))
        args = [p_star, w, theta, rest, g, eta, inv, v_part, side]
        outs = [BLOCK] * 3
        if last:
            u_far, v_far, t0, y0 = call(
                functools.partial(upward, False, True),
                [(NK, NI, NL)] + outs,
                args + [u],
                f"upward{step}",
                scratch=[vmem(*BLOCK), pltpu.SemaphoreType.DMA((1 + NK // BATCH,))],
                far_out=2,
            )
        elif first:
            t0, y0, v, b_v = call(
                functools.partial(upward, True, False), outs + [BLOCK], args + [b_v, by_first, by_second], f"upward{step}"
            )
        else:
            t0, y0, v = call(functools.partial(upward, False, False), outs, args, f"upward{step}")
        args = [t0, y0, t1, y1, eta, inv, message, by1, by2, by3]
        args += [] if first else [kept]
        body = functools.partial(implicit, first, last)
        if last:
            w_far, p_far = call(
                body,
                [BLOCK] * 2,
                args,
                f"implicit{step}",
                scratch=[vmem(*BLOCK), vmem(*BLOCK), pltpu.SemaphoreType.DMA((2 * NK // CHUNK,))],
                far_out=2,
                limit=3,
            )
        else:
            outs = [BLOCK, BLOCK, (2 * NI, NL), (2 * NK, NL), (2 * NK, NL), PACK]
            outs += [(sum(COUNTS) * NI, NL)] if first else []
            w, p, sums, to_chip, to_far, own, *fixed = call(body, outs, args + [a_w, top_w], f"implicit{step}")
            to_first = to_second = own
            if first:
                kept = fixed[0]
    return tuple(x.reshape(NK, NI, NL) for x in (u_far, v_far, w_far, p_far))


def solution(mesh):
    return jax.shard_map(
        shards,
        mesh=mesh,
        in_specs=(P("lev", "gx", "gy"),) * 6,
        out_specs=(P("lev", "gx", "gy"),) * 4,
        check_vma=False,
    )
```

```python
import functools

import jax
import jax.numpy as jnp
from jax import lax
from jax.experimental import pallas as pl
from jax.experimental.pallas import tpu as pltpu
from jax.sharding import PartitionSpec as P


SUBSTEPS = 3

courant_h = 0.3
vertical_gain = 4096.0

F32 = jnp.float32
NI, NK, NL = 16, 64, 128

STEP = 24
PADDED = ((NK + 1) * STEP, NL)
BLOCK = (NI * NK, NL)
PACK = (4 * 8, NL)


def level(k):
    return pl.ds(NI * k, NI)


def row(i):
    return pl.ds(NK * i, NK)


def padded_row(i):
    return pl.ds(8 + i, NK, stride=STEP)


def main_rows(padded):
    return padded.reshape(NK + 1, STEP, NL).at[pl.ds(0, NK), pl.ds(8, NI), :]


def vmem(*shape):
    return pltpu.VMEM(shape, F32)


def hbm(*shape):
    return pltpu.HBM(shape, F32)


def call(body, outs, args, scratch=(), aliases=None, far_in=0, far_out=0, limit=2):
    near, far = pl.BlockSpec(memory_space=pltpu.VMEM), pl.BlockSpec(memory_space=pltpu.HBM)
    args = [
        pltpu.with_memory_space_constraint(x, pltpu.HBM if at < far_in else pltpu.VMEM) for at, x in enumerate(args)
    ]
    return pl.pallas_call(
        body,
        out_shape=tuple((hbm if at < far_out else vmem)(*shape) for at, shape in enumerate(outs)),
        in_specs=[far] * far_in + [near] * (len(args) - far_in),
        out_specs=(far,) * far_out + (near,) * (len(outs) - far_out),
        scratch_shapes=list(scratch),
        input_output_aliases=aliases or {},
        compiler_params=pltpu.CompilerParams(vmem_limit_bytes=limit << 20),
    )(*args)


def tiles():
    for group in range(4):
        for tile in range(32):
            yield group, tile, group * 16 + tile // 2, 8 * (tile % 2)


def pack_edges(load):
    lane = lax.broadcasted_iota(jnp.int32, (8, NL), 1) // 4
    packs = [jnp.zeros((8, NL), F32)] * 4
    for group, tile, k, i in tiles():
        rolled = pltpu.roll(load(k, i), 4 * tile + 2, 1)
        packs[group] = jnp.where(lane == tile, rolled, packs[group])
    return jnp.concatenate(packs, 0)


def slots(shape=PACK):
    return lax.broadcasted_iota(jnp.int32, shape, 1) % 4


def turn(x, by):
    return pltpu.roll(x, by % NL, 1)


def block_row(i):
    return pl.ds(i, NK, stride=NI)


def is_even(axis):
    return (lax.axis_index(axis) & 1) == 0


def prologue(p_in, v_in, b_in, u_in, p, v, b, u, to_chip, to_far, to_right, to_left, to_first, to_second, sems):
    copies = []
    for at, (source, target) in enumerate(((p_in, p), (v_in, v), (b_in, b), (u_in, u))):
        if at == 3:
            target = main_rows(target)
        copies.append(pltpu.make_async_copy(source, target, sems.at[at]))
    for copy in copies:
        copy.start()
    packs = []
    for copy, field in zip(copies, (p, v, b)):
        copy.wait()
        packs.append(pack_edges(lambda k, i: field[pl.ds(NI * k + i, 8), :]))
    edge_p, edge_v, edge_b = packs
    slot = slots()
    going_right = jnp.where(slot < 2, edge_p, jnp.where(slot == 2, turn(edge_v, 1), turn(edge_b, 2)))
    going_left = jnp.where(slot < 2, turn(edge_p, -2), jnp.where(slot == 2, edge_v, turn(edge_b, 1)))
    to_right[...] = going_right
    to_left[...] = going_left
    even = is_even("gy")
    to_first[...] = jnp.where(even, going_right, going_left)
    to_second[...] = jnp.where(even, going_left, going_right)
    copies[3].wait()
    even = is_even("gx")
    up, down = (
        [p[block_row(edge), :], u[padded_row(edge), :] + away * courant_h * b[block_row(edge), :] * p[block_row(next_to), :]]
        + [b[block_row(edge), :]]
        for edge, next_to, away in ((NI - 1, NI - 2, 1), (0, 1, -1))
    )
    for at in range(3):
        to_chip[row(at), :] = jnp.where(even, up[at], down[at])
        to_far[row(at), :] = jnp.where(even, down[at], up[at])


def factor(
    s_in, w_in, b_in, v_in,
    theta, rest, g_out, eta, inv, t1, y1, a_p, top_p, a_w, top_w, v, b_v, statics, sums,
):
    first = s_in[level(0), :]
    passed = first
    held = None
    for k in range(NK):
        v[level(k), :] = turn(v_in[level(k), :], -1)
        b_v[level(k), :] = turn(b_in[level(k), :], -1)
        g = 1.0 / (vertical_gain * b_in[level(k), :])
        g_out[level(k), :] = g
        stiff = s_in[level(k), :]
        if k == 0:
            c = first
        else:
            ratio = 1.0 / (held + stiff)
            th = held * ratio
            rs = stiff * ratio
            theta[level(k), :] = th
            rest[level(k), :] = rs
            c = stiff * th
            passed = passed * rs
        held = g + c
        ic = 1.0 / held
        inv[level(k), :] = ic
        eta[level(k), :] = c * ic
        t1[level(k), :] = (g * ic) * passed
        y1[level(k), :] = passed * ic
    theta[level(0), :] = jnp.ones((NI, NL), F32)
    rest[level(0), :] = jnp.zeros((NI, NL), F32)
    statics[level(1), :] = passed
    statics[level(2), :] = held
    weight = jnp.ones((NI, NL), F32)
    above = jnp.zeros((NI, NL), F32)
    reply_above = None
    sum_a = jnp.zeros((NI, NL), F32)
    sum_t = jnp.zeros((NI, NL), F32)
    for k in range(NK - 1, -1, -1):
        g = g_out[level(k), :]
        w = w_in[level(k), :]
        top_p[level(k), :] = theta[level(k), :] * weight
        gw = g * weight
        top_w[level(k), :] = gw
        sum_t = sum_t + gw * w
        weight = weight * rest[level(k), :]
        reply = y1[level(k), :] - inv[level(k), :] * above
        above = t1[level(k), :] + eta[level(k), :] * above
        gr = g * reply
        a_w[level(k), :] = gr
        sum_a = sum_a - gr * w
        if reply_above is not None:
            a_p[level(k + 1), :] = reply - reply_above
        reply_above = reply
    a_p[level(0), :] = 1.0 - reply_above
    statics[level(0), :] = above
    sums[level(0), :] = sum_a
    sums[level(1), :] = sum_t


BATCH = 8
CHUNK = 8


def batches():
    for start in range(0, NK, BATCH):
        spots = range(2 * (start % 16), 2 * (start % 16) + 2 * BATCH)

        def spread(pack, by, spots=spots, group=slice(8 * (start // 16), 8 * (start // 16) + 8)):
            return jnp.concatenate([turn(pack[group, :], by - 4 * tile) for tile in spots], 0)

        yield start, pl.ds(NI * start, NI * BATCH), spread


def inner(first, p, u, v, b_u, b_v, s, u_new, v_part, star_part):
    for k in range(NK):
        rows = pl.ds(STEP * k + 8, NI)
        if k == 0:
            below = jnp.concatenate([p[pl.ds(0, 1), :], p[pl.ds(0, NI - 1), :]], 0)
        else:
            below = p[pl.ds(NI * k - 1, NI), :]
        if k == NK - 1:
            above = jnp.concatenate([p[pl.ds(NI * k + 1, NI - 1), :], p[pl.ds(NI * k, 1), :]], 0)
        else:
            above = p[pl.ds(NI * k + 1, NI), :]
        u_new[rows, :] = u[rows, :] - courant_h * b_u[level(k), :] * (above - below)
    lane = lax.broadcasted_iota(jnp.int32, (NI * BATCH, NL), 1)
    for _, rows, _ in batches():
        pressure = p[rows, :]
        p_next = jnp.where(lane >= NL - 2, 0.0, turn(pressure, -2))
        vn = v[rows, :] - courant_h * b_v[rows, :] * (p_next - pressure)
        if first:
            vn = jnp.where(lane == NL - 1, 0.0, vn)
        v_part[rows, :] = vn
        star_part[rows, :] = pressure - courant_h * s[rows, :] * (vn - jnp.where(lane < 2, 0.0, turn(vn, 2)))


def explicit(first, last, *refs):
    (p, u_old, b_u, star_part, s, a_p, top_p, sums, own, chip, far, by_first, by_second, extra), refs = refs[:14], refs[15:]
    if first:
        own_right, refs = refs[0], refs[1:]
    else:
        u_sides, refs = refs[0], refs[1:]
    u, p_star, message, side = refs[:4]
    even = is_even("gx")
    for n in (0, 1):
        away, edge, second = (1, 0, 1) if n == 0 else (-1, NI - 1, NI - 2)
        mine, other = (far, chip) if n == 0 else (chip, far)
        theirs = lambda at: jnp.where(even, mine[row(at), :], other[row(at), :])
        if first:
            near, held, b_side = theirs(0), theirs(1), theirs(2)
            held = held - away * courant_h * b_side * p[block_row(edge), :]
        else:
            near, b_side = theirs(0), u_sides[row(2 + n), :]
            held = u_sides[row(n), :] - away * courant_h * b_side * (p[block_row(edge), :] - theirs(1))
        u[padded_row(edge - away), :] = held
        if not last:
            refs[4][row(n), :] = held
            refs[4][row(2 + n), :] = b_side
        u[padded_row(edge), :] = u_old[padded_row(edge), :] - away * courant_h * b_u[block_row(edge), :] * (
            p[block_row(second), :] - near
        )
    slot = slots()
    even = is_even("gy")
    left = jnp.where(even, by_second[...], by_first[...])
    right = jnp.where(even, by_first[...], by_second[...])
    from_left = turn(left, 2)
    if first:
        mine, from_right = own[...], right
        edge = turn(mine, 2)
        v_side = jnp.where(slot == 2, left, turn(mine, 1))
        b_pack = jnp.where(slot == 2, turn(left, -1), mine)
        b_edge = jnp.where(slot == 0, turn(own_right[...], -3), turn(from_right, -2))
        b_pack = jnp.where(slot < 2, b_edge, b_pack)
        ahead = turn(from_right, -1) - courant_h * b_edge * (from_right - own_right[...])
        taken = jnp.where(slot == 0, courant_h * b_edge * from_right, -ahead)
    else:
        edge = own[...]
        v_side, b_pack = extra[pl.ds(0, 32), :], extra[pl.ds(32, 32), :]
        taken = courant_h * b_pack * turn(right, -2)
    v_side = v_side - courant_h * b_pack * (edge - from_left)
    packed = jnp.where(slot < 2, taken, v_side)
    side[pl.ds(0, 32), :] = packed
    if not last:
        side[pl.ds(32, 32), :] = b_pack
    lane = lax.broadcasted_iota(jnp.int32, (NI * BATCH, NL), 1)
    at_edge = (lane < 2) | (lane >= NL - 2)
    total_a, total_t = sums[level(0), :], sums[level(1), :]
    for start, rows, spread in batches():
        du = jnp.concatenate(
            [
                u[pl.ds(STEP * k + 9, NI), :] - u[pl.ds(STEP * k + 7, NI), :]
                for k in range(start, start + BATCH)
            ],
            0,
        )
        star = star_part[rows, :] - courant_h * s[rows, :] * (du - jnp.where(at_edge, spread(packed, -2), 0.0))
        p_star[rows, :] = star
        part_a, part_t = a_p[rows, :] * star, top_p[rows, :] * star
        for k in range(BATCH):
            total_a = total_a + part_a[NI * k : NI * k + NI]
            total_t = total_t + part_t[NI * k : NI * k + NI]
    message[level(0), :] = total_a
    message[level(1), :] = total_t
    if first:
        message[pl.ds(2 * NI, 3 * NI), :] = extra[...]


def upward(first, last, *refs):
    (p_star, w, theta, rest, g_in, eta, inv, v_part, side), refs = refs[:9], refs[9:]
    copies = []
    if last:
        u, u_far, v_far, t0, y0, v_out, sems = refs

        def send(source, target):
            copies.append(pltpu.make_async_copy(source, target, sems.at[len(copies)]))
            copies[-1].start()

        send(main_rows(u), u_far)
    elif first:
        b_v, by_first, by_second, t0, y0, v_out, b_patched = refs
        right = jnp.where(is_even("gy"), by_first[...], by_second[...])
    else:
        t0, y0, v_out = refs
    lane = lax.broadcasted_iota(jnp.int32, (NI * BATCH, NL), 1)
    for _, rows, spread in batches():
        vn = v_part[rows, :] - jnp.where(lane >= NL - 2, spread(side, -2), 0.0)
        if last:
            vn = turn(jnp.where(lane == NL - 1, spread(side, -4), vn), 1)
        v_out[rows, :] = vn
        if last:
            send(v_out.at[rows, :], v_far.at[rows, :])
        if first:
            b_patched[rows, :] = jnp.where(lane == NL - 1, spread(right, NL - 4), b_v[rows, :])
    carried = held_gw = None
    for k in range(NK):
        star = p_star[level(k), :]
        gw = g_in[level(k), :] * w[level(k), :]
        if k == 0:
            carried = star
        else:
            carried = theta[level(k), :] * star + rest[level(k), :] * (carried + held_gw)
        held_gw = gw
        e = eta[level(k), :]
        t0[level(k), :] = carried - e * (carried + gw)
        y0[level(k), :] = (carried + gw) * inv[level(k), :]
    for copy in copies:
        copy.wait()


def interface(position, by_group, statics):
    a = [x[0:NI] for x in by_group]
    top = [x[NI : 2 * NI] for x in by_group]
    kappa, scale, shifted, reach, conduct = statics
    tops = [top[0]]
    for m in range(2):
        tops.append(scale[m] * top[m + 1] + shifted[m] * (tops[m] - a[m + 1]))
    y_above = jnp.zeros((NI, NL), F32)
    xs, ys = [None] * 3, [None] * 3
    for m in (2, 1, 0):
        xs[m] = kappa[m] * (tops[m] - a[m + 1] - (reach[m] * y_above if m < 2 else 0.0))
        ys[m] = tops[m] - conduct[m] * xs[m]
        y_above = ys[m]
    zero = jnp.zeros((NI, NL), F32)
    w_low = jnp.where(position == 0, zero, jnp.where(position == 1, xs[0], jnp.where(position == 2, xs[1], xs[2])))
    p_high = jnp.where(position == 3, zero, jnp.where(position == 2, ys[2], jnp.where(position == 1, ys[1], ys[0])))
    return w_low, p_high


def reduced_statics(by_group):
    beta = [x[2 * NI : 3 * NI] for x in by_group]
    phi = [x[3 * NI : 4 * NI] for x in by_group]
    grounded = [x[4 * NI : 5 * NI] for x in by_group]
    conduct = [grounded[0]]
    kappa, scale, shifted, reach = [], [], [], []
    for m in range(3):
        kappa.append(1.0 / (conduct[m] + beta[m + 1]))
        reach.append(phi[m + 1] / grounded[m + 1])
        if m < 2:
            coupled = phi[m + 1] * kappa[m]
            scale.append(1.0 / (1.0 + coupled * reach[m]))
            shifted.append(coupled * scale[m])
            conduct.append(grounded[m + 1] * scale[m])
    return kappa, scale, shifted, reach, conduct


COUNTS = (3, 2, 2, 3, 3)


def implicit(first, last, *refs):
    (t0, y0, t1, y1, eta, inv, own, by1, by2, by3), refs = refs[:10], refs[10:]
    if not first:
        kept, refs = refs[0], refs[1:]
    if last:
        w_far, p_far, w, p, sems = refs
    else:
        (a_w, top_w), (w, p, sums, to_chip, to_far, edges), refs = refs[:2], refs[2:8], refs[8:]
    position = lax.axis_index("lev")
    others = [ref[...] for ref in (own, by1, by2, by3)]
    by_group = []
    for group in range(4):
        mask = position ^ group
        by_group.append(
            jnp.where(mask == 0, others[0], jnp.where(mask == 1, others[1], jnp.where(mask == 2, others[2], others[3])))
        )
    if first:
        statics = reduced_statics(by_group)
        keep, at = refs[0], 0
        for family in statics:
            for member in family:
                keep[level(at), :] = member
                at += 1
    else:
        statics, at = [], 0
        for count in COUNTS:
            statics.append([kept[level(at + m), :] for m in range(count)])
            at += count
    w_low, p_high = interface(position, by_group, statics)
    above = p_high
    sum_a = jnp.zeros((NI, NL), F32)
    sum_t = jnp.zeros((NI, NL), F32)
    copies = []
    for k in range(NK - 1, -1, -1):
        wn = y0[level(k), :] + y1[level(k), :] * w_low - inv[level(k), :] * above
        above = t0[level(k), :] + t1[level(k), :] * w_low + eta[level(k), :] * above
        w[level(k), :] = wn
        p[level(k), :] = above
        if last:
            if k % CHUNK == 0:
                part = pl.ds(NI * k, NI * CHUNK)
                for source, target in ((w, w_far), (p, p_far)):
                    copy = pltpu.make_async_copy(source.at[part, :], target.at[part, :], sems.at[len(copies)])
                    copy.start()
                    copies.append(copy)
        else:
            sum_a = sum_a - a_w[level(k), :] * wn
            sum_t = sum_t + top_w[level(k), :] * wn
    for copy in copies:
        copy.wait()
    if not last:
        sums[level(0), :] = sum_a
        sums[level(1), :] = sum_t
        even = is_even("gx")
        for at, (i, j) in enumerate(((NI - 1, 0), (NI - 2, 1))):
            up, down = p[block_row(i), :], p[block_row(j), :]
            to_chip[row(at), :] = jnp.where(even, up, down)
            to_far[row(at), :] = jnp.where(even, down, up)
        edges[...] = pack_edges(lambda k, i: p[pl.ds(NI * k + i, 8), :])


def swap(block, axis, first):
    size = lax.axis_size(axis)
    pairs = [(i, (i + 1) % size) for i in range(first, size, 2)]
    return lax.ppermute(block, axis, pairs + [(j, i) for i, j in pairs])


def partner(block, mask):
    return lax.ppermute(block, "lev", [(i, i ^ mask) for i in range(4)])


def shards(u_wind, v_wind, w_wind, pressure, buoyancy, stiffness):
    w, s = w_wind.reshape(BLOCK), stiffness.reshape(BLOCK)
    p, v, b, u, to_chip, to_far, to_right, own, to_first, to_second = call(
        prologue,
        [BLOCK] * 3 + [PADDED, (3 * NK, NL), (3 * NK, NL)] + [PACK] * 4,
        [x.reshape(BLOCK) for x in (pressure, v_wind, buoyancy)] + [u_wind],
        scratch=[pltpu.SemaphoreType.DMA((4,))],
        far_in=4,
    )
    (theta, rest, g, eta, inv, t1, y1, a_p, top_p, a_w, top_w, v, b_v, statics, sums) = call(
        factor, [BLOCK] * 13 + [(3 * NI, NL), (2 * NI, NL)], [s, w, b, v]
    )
    side, more = statics, [to_right]
    for step in range(SUBSTEPS):
        first, last = step == 0, step == SUBSTEPS - 1
        chip = swap(to_chip, "gx", 0)
        far = swap(to_far, "gx", 1)
        by_first = swap(to_first, "gy", 0)
        by_second = swap(to_second, "gy", 1)
        u_part, v_part, star_part = call(functools.partial(inner, first), [PADDED, BLOCK, BLOCK], [p, u, v, b, b_v, s])
        args = [p, u, b, star_part, s, a_p, top_p, sums, own, chip, far, by_first, by_second, side, u_part] + more
        outs = [PADDED, BLOCK, ((5 if first else 2) * NI, NL)]
        outs += [PACK] if last else [(2 * PACK[0], NL), (4 * NK, NL)]
        u, p_star, message, side, *more = call(functools.partial(explicit, first, last), outs, args, aliases={14: 0})
        partners = []
        for mask in (1, 2, 3):
            partners.append(partner(message, mask))
        by1, by2, by3 = partners
        args = [p_star, w, theta, rest, g, eta, inv, v_part, side]
        outs = [BLOCK] * 3
        if last:
            u_far, v_far, t0, y0 = call(
                functools.partial(upward, False, True),
                [(NK, NI, NL)] + outs,
                args + [u],
                scratch=[vmem(*BLOCK), pltpu.SemaphoreType.DMA((1 + NK // BATCH,))],
                far_out=2,
            )
        elif first:
            t0, y0, v, b_v = call(
                functools.partial(upward, True, False), outs + [BLOCK], args + [b_v, by_first, by_second]
            )
        else:
            t0, y0, v = call(functools.partial(upward, False, False), outs, args)
        args = [t0, y0, t1, y1, eta, inv, message, by1, by2, by3]
        args += [] if first else [kept]
        body = functools.partial(implicit, first, last)
        if last:
            w_far, p_far = call(
                body,
                [BLOCK] * 2,
                args,
                scratch=[vmem(*BLOCK), vmem(*BLOCK), pltpu.SemaphoreType.DMA((2 * NK // CHUNK,))],
                far_out=2,
                limit=3,
            )
        else:
            outs = [BLOCK, BLOCK, (2 * NI, NL), (2 * NK, NL), (2 * NK, NL), PACK]
            outs += [(sum(COUNTS) * NI, NL)] if first else []
            w, p, sums, to_chip, to_far, own, *fixed = call(body, outs, args + [a_w, top_w])
            to_first = to_second = own
            if first:
                kept = fixed[0]
    return tuple(x.reshape(NK, NI, NL) for x in (u_far, v_far, w_far, p_far))


def solution(mesh):
    return jax.shard_map(
        shards,
        mesh=mesh,
        in_specs=(P("lev", "gx", "gy"),) * 6,
        out_specs=(P("lev", "gx", "gy"),) * 4,
        check_vma=False,
    )
```

```python
import functools

import jax
import jax.numpy as jnp
from jax import lax
from jax.experimental import pallas as pl
from jax.experimental.pallas import tpu as pltpu
from jax.sharding import PartitionSpec as P


SUBSTEPS = 3

courant_h = 0.3
vertical_gain = 4096.0

F32 = jnp.float32
NI, NK, NL = 16, 64, 128

STEP = 24
PADDED = ((NK + 1) * STEP, NL)
BLOCK = (NI * NK, NL)
PACK = (4 * 8, NL)


def level(k):
    return pl.ds(NI * k, NI)


def row(i):
    return pl.ds(NK * i, NK)


def padded_row(i):
    return pl.ds(8 + i, NK, stride=STEP)


def main_rows(padded):
    return padded.reshape(NK + 1, STEP, NL).at[pl.ds(0, NK), pl.ds(8, NI), :]


def vmem(*shape):
    return pltpu.VMEM(shape, F32)


def hbm(*shape):
    return pltpu.HBM(shape, F32)


def call(body, outs, args, scratch=(), aliases=None, far_in=0, far_out=0, limit=2):
    near, far = pl.BlockSpec(memory_space=pltpu.VMEM), pl.BlockSpec(memory_space=pltpu.HBM)
    args = [
        pltpu.with_memory_space_constraint(x, pltpu.HBM if at < far_in else pltpu.VMEM) for at, x in enumerate(args)
    ]
    return pl.pallas_call(
        body,
        out_shape=tuple((hbm if at < far_out else vmem)(*shape) for at, shape in enumerate(outs)),
        in_specs=[far] * far_in + [near] * (len(args) - far_in),
        out_specs=(far,) * far_out + (near,) * (len(outs) - far_out),
        scratch_shapes=list(scratch),
        input_output_aliases=aliases or {},
        compiler_params=pltpu.CompilerParams(vmem_limit_bytes=limit << 20),
    )(*args)


def tiles():
    for group in range(4):
        for tile in range(32):
            yield group, tile, group * 16 + tile // 2, 8 * (tile % 2)


def pack_edges(load):
    lane = lax.broadcasted_iota(jnp.int32, (8, NL), 1) // 4
    packs = [jnp.zeros((8, NL), F32)] * 4
    for group, tile, k, i in tiles():
        rolled = pltpu.roll(load(k, i), 4 * tile + 2, 1)
        packs[group] = jnp.where(lane == tile, rolled, packs[group])
    return jnp.concatenate(packs, 0)


def slots(shape=PACK):
    return lax.broadcasted_iota(jnp.int32, shape, 1) % 4


def turn(x, by):
    return pltpu.roll(x, by % NL, 1)


def block_row(i):
    return pl.ds(i, NK, stride=NI)


def is_even(axis):
    return (lax.axis_index(axis) & 1) == 0


def prologue(p_in, v_in, b_in, u_in, p, v, b, u, to_chip, to_far, to_right, to_left, to_first, to_second, sems):
    copies = []
    for at, (source, target) in enumerate(((p_in, p), (v_in, v), (b_in, b), (u_in, u))):
        if at == 3:
            target = main_rows(target)
        copies.append(pltpu.make_async_copy(source, target, sems.at[at]))
    for copy in copies:
        copy.start()
    packs = []
    for copy, field in zip(copies, (p, v, b)):
        copy.wait()
        packs.append(pack_edges(lambda k, i: field[pl.ds(NI * k + i, 8), :]))
    edge_p, edge_v, edge_b = packs
    slot = slots()
    going_right = jnp.where(slot < 2, edge_p, jnp.where(slot == 2, turn(edge_v, 1), turn(edge_b, 2)))
    going_left = jnp.where(slot < 2, turn(edge_p, -2), jnp.where(slot == 2, edge_v, turn(edge_b, 1)))
    to_right[...] = going_right
    to_left[...] = going_left
    even = is_even("gy")
    to_first[...] = jnp.where(even, going_right, going_left)
    to_second[...] = jnp.where(even, going_left, going_right)
    copies[3].wait()
    even = is_even("gx")
    up, down = (
        [p[block_row(edge), :], u[padded_row(edge), :] + away * courant_h * b[block_row(edge), :] * p[block_row(next_to), :]]
        + [b[block_row(edge), :]]
        for edge, next_to, away in ((NI - 1, NI - 2, 1), (0, 1, -1))
    )
    for at in range(3):
        to_chip[row(at), :] = jnp.where(even, up[at], down[at])
        to_far[row(at), :] = jnp.where(even, down[at], up[at])


def factor(
    s_in, w_in, b_in, v_in,
    theta, rest, g_out, eta, inv, t1, y1, a_p, top_p, a_w, top_w, v, b_v, statics, sums,
):
    first = s_in[level(0), :]
    passed = first
    held = None
    for k in range(NK):
        v[level(k), :] = turn(v_in[level(k), :], -1)
        b_v[level(k), :] = turn(b_in[level(k), :], -1)
        g = 1.0 / (vertical_gain * b_in[level(k), :])
        g_out[level(k), :] = g
        stiff = s_in[level(k), :]
        if k == 0:
            c = first
        else:
            ratio = 1.0 / (held + stiff)
            th = held * ratio
            rs = stiff * ratio
            theta[level(k), :] = th
            rest[level(k), :] = rs
            c = stiff * th
            passed = passed * rs
        held = g + c
        ic = 1.0 / held
        inv[level(k), :] = ic
        eta[level(k), :] = c * ic
        t1[level(k), :] = (g * ic) * passed
        y1[level(k), :] = passed * ic
    theta[level(0), :] = jnp.ones((NI, NL), F32)
    rest[level(0), :] = jnp.zeros((NI, NL), F32)
    statics[level(1), :] = passed
    statics[level(2), :] = held
    weight = jnp.ones((NI, NL), F32)
    above = jnp.zeros((NI, NL), F32)
    reply_above = None
    sum_a = jnp.zeros((NI, NL), F32)
    sum_t = jnp.zeros((NI, NL), F32)
    for k in range(NK - 1, -1, -1):
        g = g_out[level(k), :]
        w = w_in[level(k), :]
        top_p[level(k), :] = theta[level(k), :] * weight
        gw = g * weight
        top_w[level(k), :] = gw
        sum_t = sum_t + gw * w
        weight = weight * rest[level(k), :]
        reply = y1[level(k), :] - inv[level(k), :] * above
        above = t1[level(k), :] + eta[level(k), :] * above
        gr = g * reply
        a_w[level(k), :] = gr
        sum_a = sum_a - gr * w
        if reply_above is not None:
            a_p[level(k + 1), :] = reply - reply_above
        reply_above = reply
    a_p[level(0), :] = 1.0 - reply_above
    statics[level(0), :] = above
    sums[level(0), :] = sum_a
    sums[level(1), :] = sum_t


BATCH = 8
CHUNK = 8


def batches():
    for start in range(0, NK, BATCH):
        spots = range(2 * (start % 16), 2 * (start % 16) + 2 * BATCH)

        def spread(pack, by, spots=spots, group=slice(8 * (start // 16), 8 * (start // 16) + 8)):
            return jnp.concatenate([turn(pack[group, :], by - 4 * tile) for tile in spots], 0)

        yield start, pl.ds(NI * start, NI * BATCH), spread


def inner(first, p, u, v, b_u, b_v, s, *refs):
    if first:
        u_new, v_part, star_part = refs
    else:
        w, a_w, top_w, u_new, v_part, star_part, sums = refs
        sum_a = sum_t = jnp.zeros((NI, NL), F32)
        for k in range(NK - 1, -1, -1):
            sum_a = sum_a - a_w[level(k), :] * w[level(k), :]
            sum_t = sum_t + top_w[level(k), :] * w[level(k), :]
        sums[level(0), :] = sum_a
        sums[level(1), :] = sum_t
    for k in range(NK):
        rows = pl.ds(STEP * k + 8, NI)
        if k == 0:
            below = jnp.concatenate([p[pl.ds(0, 1), :], p[pl.ds(0, NI - 1), :]], 0)
        else:
            below = p[pl.ds(NI * k - 1, NI), :]
        if k == NK - 1:
            above = jnp.concatenate([p[pl.ds(NI * k + 1, NI - 1), :], p[pl.ds(NI * k, 1), :]], 0)
        else:
            above = p[pl.ds(NI * k + 1, NI), :]
        u_new[rows, :] = u[rows, :] - courant_h * b_u[level(k), :] * (above - below)
    lane = lax.broadcasted_iota(jnp.int32, (NI * BATCH, NL), 1)
    for _, rows, _ in batches():
        pressure = p[rows, :]
        p_next = jnp.where(lane >= NL - 2, 0.0, turn(pressure, -2))
        vn = v[rows, :] - courant_h * b_v[rows, :] * (p_next - pressure)
        if first:
            vn = jnp.where(lane == NL - 1, 0.0, vn)
        v_part[rows, :] = vn
        star_part[rows, :] = pressure - courant_h * s[rows, :] * (vn - jnp.where(lane < 2, 0.0, turn(vn, 2)))


def explicit(first, last, *refs):
    (p, u_old, b_u, star_part, s, a_p, top_p, sums, own, chip, far, by_first, by_second, extra), refs = refs[:14], refs[15:]
    if first:
        own_right, refs = refs[0], refs[1:]
    else:
        u_sides, refs = refs[0], refs[1:]
    u, p_star, message, side = refs[:4]
    even = is_even("gx")
    for n in (0, 1):
        away, edge, second = (1, 0, 1) if n == 0 else (-1, NI - 1, NI - 2)
        mine, other = (far, chip) if n == 0 else (chip, far)
        theirs = lambda at: jnp.where(even, mine[row(at), :], other[row(at), :])
        if first:
            near, held, b_side = theirs(0), theirs(1), theirs(2)
            held = held - away * courant_h * b_side * p[block_row(edge), :]
        else:
            near, b_side = theirs(0), u_sides[row(2 + n), :]
            held = u_sides[row(n), :] - away * courant_h * b_side * (p[block_row(edge), :] - theirs(1))
        u[padded_row(edge - away), :] = held
        if not last:
            refs[4][row(n), :] = held
            refs[4][row(2 + n), :] = b_side
        u[padded_row(edge), :] = u_old[padded_row(edge), :] - away * courant_h * b_u[block_row(edge), :] * (
            p[block_row(second), :] - near
        )
    slot = slots()
    even = is_even("gy")
    left = jnp.where(even, by_second[...], by_first[...])
    right = jnp.where(even, by_first[...], by_second[...])
    from_left = turn(left, 2)
    if first:
        mine, from_right = own[...], right
        edge = turn(mine, 2)
        v_side = jnp.where(slot == 2, left, turn(mine, 1))
        b_pack = jnp.where(slot == 2, turn(left, -1), mine)
        b_edge = jnp.where(slot == 0, turn(own_right[...], -3), turn(from_right, -2))
        b_pack = jnp.where(slot < 2, b_edge, b_pack)
        ahead = turn(from_right, -1) - courant_h * b_edge * (from_right - own_right[...])
        taken = jnp.where(slot == 0, courant_h * b_edge * from_right, -ahead)
    else:
        edge = own[...]
        v_side, b_pack = extra[pl.ds(0, 32), :], extra[pl.ds(32, 32), :]
        taken = courant_h * b_pack * turn(right, -2)
    v_side = v_side - courant_h * b_pack * (edge - from_left)
    packed = jnp.where(slot < 2, taken, v_side)
    side[pl.ds(0, 32), :] = packed
    if not last:
        side[pl.ds(32, 32), :] = b_pack
    lane = lax.broadcasted_iota(jnp.int32, (NI * BATCH, NL), 1)
    at_edge = (lane < 2) | (lane >= NL - 2)
    total_a, total_t = sums[level(0), :], sums[level(1), :]
    for start, rows, spread in batches():
        du = jnp.concatenate(
            [
                u[pl.ds(STEP * k + 9, NI), :] - u[pl.ds(STEP * k + 7, NI), :]
                for k in range(start, start + BATCH)
            ],
            0,
        )
        star = star_part[rows, :] - courant_h * s[rows, :] * (du - jnp.where(at_edge, spread(packed, -2), 0.0))
        p_star[rows, :] = star
        part_a, part_t = a_p[rows, :] * star, top_p[rows, :] * star
        for k in range(BATCH):
            total_a = total_a + part_a[NI * k : NI * k + NI]
            total_t = total_t + part_t[NI * k : NI * k + NI]
    message[level(0), :] = total_a
    message[level(1), :] = total_t
    if first:
        message[pl.ds(2 * NI, 3 * NI), :] = extra[...]


def upward(first, last, *refs):
    (p_star, w, theta, rest, g_in, eta, inv, v_part, side), refs = refs[:9], refs[9:]
    copies = []
    if last:
        u, u_far, v_far, t0, y0, v_out, sems = refs

        def send(source, target):
            copies.append(pltpu.make_async_copy(source, target, sems.at[len(copies)]))
            copies[-1].start()

        send(main_rows(u), u_far)
    elif first:
        b_v, by_first, by_second, t0, y0, v_out, b_patched = refs
        right = jnp.where(is_even("gy"), by_first[...], by_second[...])
    else:
        t0, y0, v_out = refs
    lane = lax.broadcasted_iota(jnp.int32, (NI * BATCH, NL), 1)
    for _, rows, spread in batches():
        vn = v_part[rows, :] - jnp.where(lane >= NL - 2, spread(side, -2), 0.0)
        if last:
            vn = turn(jnp.where(lane == NL - 1, spread(side, -4), vn), 1)
        v_out[rows, :] = vn
        if last:
            send(v_out.at[rows, :], v_far.at[rows, :])
        if first:
            b_patched[rows, :] = jnp.where(lane == NL - 1, spread(right, NL - 4), b_v[rows, :])
    carried = held_gw = None
    for k in range(NK):
        star = p_star[level(k), :]
        gw = g_in[level(k), :] * w[level(k), :]
        if k == 0:
            carried = star
        else:
            carried = theta[level(k), :] * star + rest[level(k), :] * (carried + held_gw)
        held_gw = gw
        e = eta[level(k), :]
        t0[level(k), :] = carried - e * (carried + gw)
        y0[level(k), :] = (carried + gw) * inv[level(k), :]
    for copy in copies:
        copy.wait()


def interface(position, by_group, statics):
    a = [x[0:NI] for x in by_group]
    top = [x[NI : 2 * NI] for x in by_group]
    kappa, scale, shifted, reach, conduct = statics
    tops = [top[0]]
    for m in range(2):
        tops.append(scale[m] * top[m + 1] + shifted[m] * (tops[m] - a[m + 1]))
    y_above = jnp.zeros((NI, NL), F32)
    xs, ys = [None] * 3, [None] * 3
    for m in (2, 1, 0):
        xs[m] = kappa[m] * (tops[m] - a[m + 1] - (reach[m] * y_above if m < 2 else 0.0))
        ys[m] = tops[m] - conduct[m] * xs[m]
        y_above = ys[m]
    zero = jnp.zeros((NI, NL), F32)
    w_low = jnp.where(position == 0, zero, jnp.where(position == 1, xs[0], jnp.where(position == 2, xs[1], xs[2])))
    p_high = jnp.where(position == 3, zero, jnp.where(position == 2, ys[2], jnp.where(position == 1, ys[1], ys[0])))
    return w_low, p_high


def reduced_statics(by_group):
    beta = [x[2 * NI : 3 * NI] for x in by_group]
    phi = [x[3 * NI : 4 * NI] for x in by_group]
    grounded = [x[4 * NI : 5 * NI] for x in by_group]
    conduct = [grounded[0]]
    kappa, scale, shifted, reach = [], [], [], []
    for m in range(3):
        kappa.append(1.0 / (conduct[m] + beta[m + 1]))
        reach.append(phi[m + 1] / grounded[m + 1])
        if m < 2:
            coupled = phi[m + 1] * kappa[m]
            scale.append(1.0 / (1.0 + coupled * reach[m]))
            shifted.append(coupled * scale[m])
            conduct.append(grounded[m + 1] * scale[m])
    return kappa, scale, shifted, reach, conduct


COUNTS = (3, 2, 2, 3, 3)


def implicit(first, last, *refs):
    (t0, y0, t1, y1, eta, inv, own, by1, by2, by3), refs = refs[:10], refs[10:]
    if not first:
        kept, refs = refs[0], refs[1:]
    if last:
        w_far, p_far, w, p, sems = refs
    else:
        (w, p, to_chip, to_far, edges), refs = refs[:5], refs[5:]
    position = lax.axis_index("lev")
    others = [ref[...] for ref in (own, by1, by2, by3)]
    by_group = []
    for group in range(4):
        mask = position ^ group
        by_group.append(
            jnp.where(mask == 0, others[0], jnp.where(mask == 1, others[1], jnp.where(mask == 2, others[2], others[3])))
        )
    if first:
        statics = reduced_statics(by_group)
        keep, at = refs[0], 0
        for family in statics:
            for member in family:
                keep[level(at), :] = member
                at += 1
    else:
        statics, at = [], 0
        for count in COUNTS:
            statics.append([kept[level(at + m), :] for m in range(count)])
            at += count
    w_low, p_high = interface(position, by_group, statics)
    above = p_high
    copies = []
    for k in range(NK - 1, -1, -1):
        wn = y0[level(k), :] + y1[level(k), :] * w_low - inv[level(k), :] * above
        above = t0[level(k), :] + t1[level(k), :] * w_low + eta[level(k), :] * above
        w[level(k), :] = wn
        p[level(k), :] = above
        if last:
            if k % CHUNK == 0:
                part = pl.ds(NI * k, NI * CHUNK)
                for source, target in ((w, w_far), (p, p_far)):
                    copy = pltpu.make_async_copy(source.at[part, :], target.at[part, :], sems.at[len(copies)])
                    copy.start()
                    copies.append(copy)
    for copy in copies:
        copy.wait()
    if not last:
        even = is_even("gx")
        for at, (i, j) in enumerate(((NI - 1, 0), (NI - 2, 1))):
            up, down = p[block_row(i), :], p[block_row(j), :]
            to_chip[row(at), :] = jnp.where(even, up, down)
            to_far[row(at), :] = jnp.where(even, down, up)
        edges[...] = pack_edges(lambda k, i: p[pl.ds(NI * k + i, 8), :])


def swap(block, axis, first):
    size = lax.axis_size(axis)
    pairs = [(i, (i + 1) % size) for i in range(first, size, 2)]
    return lax.ppermute(block, axis, pairs + [(j, i) for i, j in pairs])


def partner(block, mask):
    return lax.ppermute(block, "lev", [(i, i ^ mask) for i in range(4)])


def shards(u_wind, v_wind, w_wind, pressure, buoyancy, stiffness):
    w, s = w_wind.reshape(BLOCK), stiffness.reshape(BLOCK)
    p, v, b, u, to_chip, to_far, to_right, own, to_first, to_second = call(
        prologue,
        [BLOCK] * 3 + [PADDED, (3 * NK, NL), (3 * NK, NL)] + [PACK] * 4,
        [x.reshape(BLOCK) for x in (pressure, v_wind, buoyancy)] + [u_wind],
        scratch=[pltpu.SemaphoreType.DMA((4,))],
        far_in=4,
    )
    (theta, rest, g, eta, inv, t1, y1, a_p, top_p, a_w, top_w, v, b_v, statics, sums) = call(
        factor, [BLOCK] * 13 + [(3 * NI, NL), (2 * NI, NL)], [s, w, b, v]
    )
    side, more = statics, [to_right]
    for step in range(SUBSTEPS):
        first, last = step == 0, step == SUBSTEPS - 1
        chip = swap(to_chip, "gx", 0)
        far = swap(to_far, "gx", 1)
        by_first = swap(to_first, "gy", 0)
        by_second = swap(to_second, "gy", 1)
        u_part, v_part, star_part, *fresh = call(
            functools.partial(inner, first),
            [PADDED, BLOCK, BLOCK] + ([] if first else [(2 * NI, NL)]),
            [p, u, v, b, b_v, s] + ([] if first else [w, a_w, top_w]),
        )
        if not first:
            sums = fresh[0]
        args = [p, u, b, star_part, s, a_p, top_p, sums, own, chip, far, by_first, by_second, side, u_part] + more
        outs = [PADDED, BLOCK, ((5 if first else 2) * NI, NL)]
        outs += [PACK] if last else [(2 * PACK[0], NL), (4 * NK, NL)]
        u, p_star, message, side, *more = call(functools.partial(explicit, first, last), outs, args, aliases={14: 0})
        partners = []
        for mask in (1, 2, 3):
            partners.append(partner(message, mask))
        by1, by2, by3 = partners
        args = [p_star, w, theta, rest, g, eta, inv, v_part, side]
        outs = [BLOCK] * 3
        if last:
            u_far, v_far, t0, y0 = call(
                functools.partial(upward, False, True),
                [(NK, NI, NL)] + outs,
                args + [u],
                scratch=[vmem(*BLOCK), pltpu.SemaphoreType.DMA((1 + NK // BATCH,))],
                far_out=2,
            )
        elif first:
            t0, y0, v, b_v = call(
                functools.partial(upward, True, False), outs + [BLOCK], args + [b_v, by_first, by_second]
            )
        else:
            t0, y0, v = call(functools.partial(upward, False, False), outs, args)
        args = [t0, y0, t1, y1, eta, inv, message, by1, by2, by3]
        args += [] if first else [kept]
        body = functools.partial(implicit, first, last)
        if last:
            w_far, p_far = call(
                body,
                [BLOCK] * 2,
                args,
                scratch=[vmem(*BLOCK), vmem(*BLOCK), pltpu.SemaphoreType.DMA((2 * NK // CHUNK,))],
                far_out=2,
                limit=3,
            )
        else:
            outs = [BLOCK, BLOCK, (2 * NK, NL), (2 * NK, NL), PACK]
            outs += [(sum(COUNTS) * NI, NL)] if first else []
            w, p, to_chip, to_far, own, *fixed = call(body, outs, args)
            to_first = to_second = own
            if first:
                kept = fixed[0]
    return tuple(x.reshape(NK, NI, NL) for x in (u_far, v_far, w_far, p_far))


def solution(mesh):
    return jax.shard_map(
        shards,
        mesh=mesh,
        in_specs=(P("lev", "gx", "gy"),) * 6,
        out_specs=(P("lev", "gx", "gy"),) * 4,
        check_vma=False,
    )
```
